32 devices in a mesh: grp: 2 (over y), gy: 4 (over z), gx: 2 (over x), gz: 2 (over core).
Axes of the slice: x: 2, y: 2, z: 4, core: 2. Of those that a mesh axis runs over, the one named last changes fastest.
Arguments:
- pair: bfloat16 [1024, 512, 128], P(('grp', 'gx', 'gz'), 'gy'), parts along dimension 0, may hold values from -6 to 6
- lengths: int32 [2], P('grp'), parts along dimension 0, may hold values from 256 to 512
- ln_gain: float32 [128], replicated, may hold values from 0.1 to 1.9
- ln_bias: float32 [128], replicated, may hold values from -3 to 3
- w_ab: bfloat16 [128, 512], replicated, may hold values from -0.5 to 0.5
- w_gate: bfloat16 [128, 128], replicated, may hold values from -0.5 to 0.5
- out_gain: float32 [128], replicated, may hold values from 0.1 to 1.9
- out_bias: float32 [128], replicated, may hold values from -3 to 3
- w_out: bfloat16 [128, 128], replicated, may hold values from -0.5 to 0.5
Outputs:
- update: bfloat16 [1024, 512, 128], P(('grp', 'gx', 'gz'), 'gy'), parts along dimension 0
The draws below stay inside these ranges and needn't reach their ends.
There are 2 independent parts, one for each index of `grp`. The reference program is written for one: setup_inputs(seed, part) draws one part's arguments, and reference() takes and returns one part's arrays. A program takes and returns all parts, laid end to end along the dimension named above; an argument that names none is the same for every part. Nothing has to cross between parts.
Inputs may be any that keep to these rules, and one draw needn't show every extreme that they name: Residues from lengths[0] on are padding.
All inputs are finite; a program needn't handle non-finite values.
Results may differ from the reference program's by a relative error of at most 0.0052.
Values may be sent and summed in bfloat16 or wider, within the bound.
A program may use at most 128 MiB of HBM per device.

```python
import jax
import jax.numpy as jnp
from jax import lax

N = 512
C = 128
CH = 128


def shard_levels(key, dims, pieces, smallest, top_value):
    factor_of, own = 1.0, jax.random.fold_in(key, 6)
    for dim, parts in pieces:
        steps = jnp.exp(jax.random.uniform(jax.random.fold_in(own, dim), (parts,), jnp.float32, smallest / len(pieces), top_value / len(pieces)))
        factor_of = factor_of * jnp.repeat(steps, dims[dim] // parts).reshape([-1 if axis == dim else 1 for axis in range(len(dims))])
    return factor_of


def gaussian(rng, extent, scale, reach, pieces=(), kind=jnp.bfloat16):
    level = shard_levels(rng, extent, pieces, -0.22, 0.18) if pieces else 1.0
    array = jax.random.normal(rng, extent, jnp.float32) * scale * level
    return jnp.minimum(jnp.maximum(array, -reach), reach).astype(kind)


def setup_inputs(seed: int = 0, part: int = 0) -> dict:
    keys = jax.random.split(jax.random.key(seed), 10)
    part_keys = jax.random.split(jax.random.fold_in(keys[9], part), 10)
    pair = gaussian(part_keys[0], (N, N, C), 1.0, 6.0, ((0, 4), (1, 4)))
    lengths = jax.random.randint(part_keys[1], (1,), N // 2, N + 1).astype(jnp.int32)
    ln_gain = jnp.clip(1.0 + 0.18 * jax.random.normal(keys[2], (C,), jnp.float32), 0.1, 1.9)
    ln_bias = gaussian(keys[3], (C,), 0.5, 3.0, (), jnp.float32)
    w_ab = gaussian(keys[4], (C, 4 * CH), C ** -0.5, 0.5)
    w_gate = gaussian(keys[5], (C, C), C ** -0.5, 0.5)
    out_gain = jnp.clip(1.0 + 0.18 * jax.random.normal(keys[6], (CH,), jnp.float32), 0.1, 1.9)
    out_bias = gaussian(keys[7], (CH,), 0.5, 3.0, (), jnp.float32)
    w_out = gaussian(keys[8], (CH, C), CH ** -0.5, 0.5)
    return dict(pair=pair, lengths=lengths, ln_gain=ln_gain, ln_bias=ln_bias, w_ab=w_ab, w_gate=w_gate, out_gain=out_gain, out_bias=out_bias, w_out=w_out)


def layer_norm(values, gain, bias):
    values = values.astype(jnp.float32)
    mean = lax.optimization_barrier(jnp.mean(values, -1, keepdims=True))
    spread = lax.optimization_barrier(jnp.mean(jnp.square(values - mean), -1, keepdims=True))
    return (values - mean) * lax.rsqrt(spread + 1e-05) * gain.astype(jnp.float32) + bias.astype(jnp.float32)

def reference(pair, lengths, ln_gain, ln_bias, w_ab, w_gate, out_gain, out_bias, w_out):
    hidden = w_out.shape[0]
    width = pair.shape[2]
    normed = layer_norm(pair, ln_gain, ln_bias).astype(jnp.bfloat16)
    flat = normed.reshape(N * N, width)
    proj = jnp.dot(flat, w_ab, preferred_element_type=jnp.float32).reshape(N, N, 4 * hidden)
    live = (jnp.arange(N, dtype=jnp.int32) < lengths[0]).astype(jnp.float32)
    pair_mask = (live[:, None] * live[None, :])[..., None]
    left = (pair_mask * jax.nn.sigmoid(proj[..., :hidden]) * proj[..., hidden:2 * hidden]).astype(jnp.bfloat16)
    right = (pair_mask * jax.nn.sigmoid(proj[..., 2 * hidden:3 * hidden]) * proj[..., 3 * hidden:]).astype(jnp.bfloat16)
    triangle = jnp.einsum('ikc,jkc->ijc', left.astype(jnp.float32), right.astype(jnp.float32), precision=lax.Precision.HIGHEST)
    tri_norm = layer_norm(triangle, out_gain, out_bias).astype(jnp.bfloat16)
    gate = jax.nn.sigmoid(jnp.dot(flat, w_gate, preferred_element_type=jnp.float32))
    projected = jnp.dot(tri_norm.reshape(N * N, hidden), w_out, preferred_element_type=jnp.float32)
    return (gate * projected).astype(jnp.bfloat16).reshape(N, N, width)
```

```python
import functools

import jax
import jax.numpy as jnp
from jax import lax
from jax.experimental import pallas as pl
from jax.experimental.pallas import tpu as pltpu
from jax.sharding import PartitionSpec as P

CHUNKS = 32
LAG = 2
DIRECT = 2
GROUPS = 4
ROWS = 32


def layer_norm(values, gain, bias):
    values = values.astype(jnp.float32)
    mean = jnp.mean(values, -1, keepdims=True)
    spread = jnp.mean(jnp.square(values - mean), -1, keepdims=True)
    return (values - mean) * lax.rsqrt(spread + 1e-05) * gain + bias


def channel_norm(values, gain, bias):
    mean = jnp.mean(values, 0, keepdims=True)
    spread = jnp.mean(jnp.square(values - mean), 0, keepdims=True)
    return (values - mean) * lax.rsqrt(spread + 1e-05) * gain[:, None, None] + bias[:, None, None]


def gather_body(pair, lengths, ln_gain, ln_bias, w_ab, w_gate, out_gain, out_bias, w_out):
    tile_rows, tile_cols, width = pair.shape
    hidden = w_out.shape[0]
    row_start = lax.axis_index(("gx", "gz")) * tile_rows
    col_index = lax.axis_index("gy")
    col_start = col_index * tile_cols
    normed = layer_norm(pair, ln_gain, ln_bias).astype(jnp.bfloat16)
    flat = normed.reshape(tile_rows * tile_cols, width)
    proj = jnp.dot(flat, w_ab, preferred_element_type=jnp.float32).reshape(
        tile_rows, tile_cols, 4 * hidden
    )
    row_live = (row_start + jnp.arange(tile_rows, dtype=jnp.int32) < lengths[0]).astype(jnp.float32)
    col_live = (col_start + jnp.arange(tile_cols, dtype=jnp.int32) < lengths[0]).astype(jnp.float32)
    pair_mask = (row_live[:, None] * col_live[None, :])[..., None]
    left = (pair_mask * jax.nn.sigmoid(proj[..., :hidden]) * proj[..., hidden : 2 * hidden]).astype(
        jnp.bfloat16
    )
    right = (
        pair_mask * jax.nn.sigmoid(proj[..., 2 * hidden : 3 * hidden]) * proj[..., 3 * hidden :]
    ).astype(jnp.bfloat16)
    left_major = jnp.transpose(left, (2, 0, 1))
    right_major = jnp.transpose(right, (2, 0, 1))
    column_rows = lax.all_gather(right_major, ("gx", "gz"), axis=1, tiled=True)
    right_mine = lax.all_to_all(column_rows, "gy", split_axis=1, concat_axis=2, tiled=True)
    triangle = jnp.einsum(
        "cik,cjk->cij",
        lax.all_gather(left_major, "gy", axis=2, tiled=True),
        right_mine,
        preferred_element_type=jnp.float32,
    )
    tri_norm = channel_norm(triangle, out_gain, out_bias).astype(jnp.bfloat16)
    gate = jax.nn.sigmoid(jnp.dot(flat, w_gate, preferred_element_type=jnp.float32)).reshape(
        tile_rows, tile_cols, width
    )
    projected = jnp.einsum("cij,cd->ijd", tri_norm, w_out, preferred_element_type=jnp.float32)
    return (gate * projected).astype(jnp.bfloat16)


def exchange_kernel(
    nx,
    nz,
    lengths,
    pair,
    gain,
    bias,
    w_ab,
    w_gate,
    out,
    gate_out,
    normed,
    send,
    gate_held,
    held,
    given,
    taken,
    operand_send,
    operand_recv,
    pass_send,
    cross_send,
    cross_recv,
    back_send,
    back_recv,
    pair_sem,
    gate_sem,
):
    nr = nx * nz
    hidden, rows, cols = send.shape[1:]
    width = pair.shape[2]
    blocks, lanes = rows // ROWS, ROWS * cols
    each = hidden // nr
    chunks = cross_recv.shape[0]
    part = each // chunks
    gy, gx, gz = lax.axis_index("gy"), lax.axis_index("gx"), lax.axis_index("gz")
    me = gx * nz + gz
    half = gy // 2
    inner_plane, outer_plane = 1 + half, 3 * half
    inner = gy == inner_plane
    outer = jnp.logical_not(inner)

    def place(tall, plane):
        return {"gy": plane, "gx": tall // nz, "gz": tall % nz}

    def remote(src, dst, send_sem, recv_sem, device):
        return pltpu.make_async_remote_copy(
            src_ref=src,
            dst_ref=dst,
            send_sem=send_sem,
            recv_sem=recv_sem,
            device_id=device,
            device_id_type=pl.DeviceIdType.MESH,
        )

    def channels(chunk):
        return pl.ds(chunk * part, part)

    def band(tall):
        return pl.ds(pl.multiple_of(tall * rows, rows), rows)

    def columns(plane):
        return pl.ds(pl.multiple_of((plane - 2 * half) * cols, cols), cols)

    def deal(chunk, step):
        peer = lax.rem(me + step, nr)
        return remote(
            send.at[:, pl.ds(peer * each + chunk * part, part)],
            held.at[:, channels(chunk), band(me), pl.ds(0, cols)],
            operand_send,
            operand_recv.at[chunk],
            place(peer, gy),
        )

    def keep_in(chunk):
        return pltpu.make_async_copy(
            send.at[:, pl.ds(me * each + chunk * part, part)],
            held.at[:, channels(chunk), band(me), pl.ds(0, cols)],
            operand_recv.at[chunk],
        )

    def pass_on(chunk):
        return remote(
            held.at[:, channels(chunk), :, pl.ds(0, cols)],
            held.at[:, channels(chunk), :, pl.ds(cols, cols)],
            pass_send,
            operand_recv.at[chunk],
            place(me, inner_plane),
        )

    def deal_inward(chunk, step):
        peer = lax.rem(me + step, nr)
        return remote(
            send.at[:, pl.ds(peer * each + chunk * part, part)],
            held.at[:, channels(chunk), band(me), pl.ds(cols, cols)],
            operand_send,
            operand_recv.at[chunk],
            place(peer, inner_plane),
        )

    def cross(chunk):
        return remote(
            given.at[channels(chunk)],
            taken.at[channels(chunk)],
            cross_send,
            cross_recv.at[chunk],
            place(me, 3 - gy),
        )

    def hand_back(chunk, step, plane):
        peer = lax.rem(me + step, nr)
        return remote(
            taken.at[channels(chunk), band(peer), columns(plane)],
            out.at[pl.ds(me * each + chunk * part, part)],
            back_send,
            back_recv,
            place(peer, plane),
        )

    def keep_out(chunk):
        return pltpu.make_async_copy(
            taken.at[channels(chunk), band(me), columns(inner_plane)],
            out.at[pl.ds(me * each + chunk * part, part)],
            back_recv,
        )

    def load(block):
        return pltpu.make_async_copy(
            pair.at[pl.ds(block * ROWS, ROWS)],
            normed.at[pl.ds(block * ROWS, ROWS)],
            pair_sem.at[block],
        )

    for block in range(blocks):
        load(block).start()
    barrier = pltpu.get_barrier_semaphore()
    total = 4 * nr
    index = gy * nr + me
    for step in range(1, total):
        peer = lax.rem(index + step, total)
        pl.semaphore_signal(
            barrier,
            inc=1,
            device_id=place(peer % nr, peer // nr),
            device_id_type=pl.DeviceIdType.MESH,
        )

    def take(ref, semaphore):
        pltpu.make_async_copy(ref, ref, semaphore).wait()

    def dealt(chunk, planes):
        take(held.at[:, channels(chunk), :, pl.ds(0, planes * cols)], operand_recv.at[chunk])

    def product(channel, which):
        below = pl.ds(pl.multiple_of(which * 2 * cols, 2 * cols), 2 * cols)
        return lax.dot_general(
            held[0, channel],
            held[1, channel, below, :],
            (((1,), (1,)), ((), ())),
            preferred_element_type=jnp.float32,
        )

    @pl.loop(0, blocks)
    def _(block):
        load(block).wait()
        here = pl.ds(pl.multiple_of(block * ROWS, ROWS), ROWS)
        flat = normed[here].reshape(lanes, width)
        value = layer_norm(flat, gain[...], bias[...]).astype(jnp.bfloat16)
        normed[here] = value.reshape(ROWS, cols, width)

    upright_w = jnp.transpose(w_ab[...].astype(jnp.float32))
    lane = lax.broadcasted_iota(jnp.int32, (1, lanes), 1)
    col_live = gy * cols + lane % cols < lengths[0]
    span = each // GROUPS

    def project(group):
        starts = [
            kind * hidden + tall * each + group * span for kind in range(4) for tall in range(nr)
        ]
        weights = jnp.concatenate([upright_w[at : at + span] for at in starts]).astype(jnp.bfloat16)
        height = nr * span

        @pl.loop(0, blocks)
        def _(block):
            here = pl.ds(pl.multiple_of(block * ROWS, ROWS), ROWS)
            proj = lax.dot_general(
                weights,
                normed[here].reshape(lanes, width),
                (((1,), (1,)), ((), ())),
                preferred_element_type=jnp.float32,
            )
            row_live = me * rows + block * ROWS + lane // cols < lengths[0]
            mask = (row_live & col_live).astype(jnp.float32)
            for side in range(2):
                gates = proj[2 * side * height : (2 * side + 1) * height]
                values = proj[(2 * side + 1) * height : (2 * side + 2) * height]
                value = mask * jax.nn.sigmoid(gates) * values
                value = value.reshape(height, ROWS, cols).astype(jnp.bfloat16)
                for tall in range(nr):
                    first = tall * each + group * span
                    send[side, first : first + span, here] = value[tall * span : (tall + 1) * span]

        if group == 0:
            pl.semaphore_wait(barrier, total - 1)

        @pl.loop(group * span // part, (group + 1) * span // part)
        def _(chunk):
            direct = outer & (chunk < DIRECT)

            @pl.when(direct)
            def _():
                for step in range(nr):
                    deal_inward(chunk, step).start()

            @pl.when(jnp.logical_not(direct))
            def _():
                for step in range(1, nr):
                    deal(chunk, step).start()
                keep_in(chunk).start()

    for group in range(GROUPS):
        project(group)
        if group:

            @pl.when(outer)
            def _():
                dealt(DIRECT + group - 1, 1)
                pass_on(DIRECT + group - 1).start()

    def store_gate(block):
        return pltpu.make_async_copy(
            gate_held.at[block % 2],
            gate_out.at[pl.ds(block * ROWS, ROWS)],
            gate_sem.at[block % 2],
        )

    def gate_turn(turn):
        block = turn - 2 * GROUPS

        @pl.when((block >= 2) & (block < blocks + 2))
        def _():
            store_gate(block - 2).wait()

        @pl.when((block >= 0) & (block < blocks))
        def _():
            here = pl.ds(pl.multiple_of(block * ROWS, ROWS), ROWS)
            value = jax.nn.sigmoid(
                jnp.dot(
                    normed[here].reshape(lanes, width),
                    w_gate[...],
                    preferred_element_type=jnp.float32,
                )
            )
            gate_held[block % 2] = value.reshape(ROWS, cols, width)
            store_gate(block).start()

    @pl.when(outer)
    def _():
        @pl.loop(DIRECT + GROUPS - 1, chunks)
        def _(chunk):
            dealt(chunk, 1)
            pass_on(chunk).start()
            gate_turn(chunk)

        take(out, back_recv)
        late = each - DIRECT * part
        take(send.at[:, pl.ds(0, nr * DIRECT * part + (nr - 1) * late)], operand_send)
        take(held.at[:, pl.ds(0, late), :, pl.ds(0, cols)], pass_send)

    @pl.when(inner)
    def _():
        @pl.loop(0, chunks + LAG)
        def _(turn):
            @pl.when(turn < chunks)
            def _():
                dealt(turn, 2)

                @pl.loop(turn * part, (turn + 1) * part)
                def _(channel):
                    given[channel] = product(channel, 1 - half).astype(jnp.bfloat16)

                cross(turn).start()

            @pl.when(turn >= LAG)
            def _():
                chunk = turn - LAG
                cross(chunk).wait_recv()

                @pl.loop(chunk * part, (chunk + 1) * part)
                def _(channel):
                    total = product(channel, half) + taken[channel].astype(jnp.float32)
                    taken[channel] = total.astype(jnp.bfloat16)

                for step in range(nr):
                    hand_back(chunk, step, outer_plane).start()
                for step in range(1, nr):
                    hand_back(chunk, step, inner_plane).start()
                keep_out(chunk).start()

            gate_turn(turn)

        take(out, back_recv)
        take(send.at[:, pl.ds(0, (nr - 1) * each)], operand_send)
        take(given, cross_send)
        take(taken.at[:, pl.ds(0, (2 * nr - 1) * rows // 2)], back_send)


def upright(row):
    return jnp.transpose(jnp.broadcast_to(row[...], (row.shape[1], row.shape[1])))[:, :1]


def finish_kernel(gate, tri, out_gain, out_bias, w_out, out):
    rows, cols, width = out.shape
    hidden = tri.shape[0]
    values = tri[...].astype(jnp.float32)
    mean = jnp.mean(values, 0, keepdims=True)
    centred = values - mean
    spread = jnp.mean(jnp.square(centred), 0, keepdims=True)
    scaled = (centred * lax.rsqrt(spread + 1e-05)).reshape(hidden, rows * cols)
    tri_norm = (scaled * upright(out_gain) + upright(out_bias)).astype(jnp.bfloat16)
    projected = lax.dot_general(
        tri_norm, w_out[...], (((0,), (0,)), ((), ())), preferred_element_type=jnp.float32
    )
    out[...] = (gate[...] * projected.reshape(rows, cols, width)).astype(jnp.bfloat16)


def whole(shape):
    return pl.BlockSpec(shape, lambda step: (0,) * len(shape))


def channel_body(sizes, pair, lengths, ln_gain, ln_bias, w_ab, w_gate, out_gain, out_bias, w_out):
    ny, nx, nz = sizes
    tile_rows, tile_cols, width = pair.shape
    hidden = w_out.shape[0]
    gain, bias = ln_gain[None, :], ln_bias[None, :]
    smem = pl.BlockSpec(memory_space=pltpu.SMEM)
    steps = tile_rows // ROWS
    dma = pltpu.SemaphoreType.DMA
    any_space = pl.BlockSpec(memory_space=pl.ANY)
    nr = nx * nz
    each, side = hidden // nr, nr * tile_rows
    vmem = pl.BlockSpec(memory_space=pltpu.VMEM)
    triangle, gate = pl.pallas_call(
        functools.partial(exchange_kernel, nx, nz),
        name="exchange",
        out_shape=(
            jax.ShapeDtypeStruct((hidden, tile_rows, tile_cols), jnp.bfloat16),
            jax.ShapeDtypeStruct(pair.shape, jnp.float32),
        ),
        in_specs=[smem, any_space, vmem, vmem, vmem, vmem],
        out_specs=(any_space, any_space),
        scratch_shapes=[
            pltpu.VMEM(pair.shape, jnp.bfloat16),
            pltpu.VMEM((2, hidden, tile_rows, tile_cols), jnp.bfloat16),
            pltpu.VMEM((2, ROWS, tile_cols, width), jnp.float32),
            pltpu.VMEM((2, each, side, 2 * tile_cols), jnp.bfloat16),
            pltpu.VMEM((each, side, 2 * tile_cols), jnp.bfloat16),
            pltpu.VMEM((each, side, 2 * tile_cols), jnp.bfloat16),
            dma,
            dma((CHUNKS,)),
            dma,
            dma,
            dma((CHUNKS,)),
            dma,
            dma,
            dma((steps,)),
            dma((2,)),
        ],
        compiler_params=pltpu.CompilerParams(
            collective_id=0, has_side_effects=True, vmem_limit_bytes=63 * 2**20
        ),
    )(lengths, pair, gain, bias, w_ab, w_gate)
    return pl.pallas_call(
        finish_kernel,
        name="finish",
        grid=(steps,),
        out_shape=jax.ShapeDtypeStruct(pair.shape, jnp.bfloat16),
        in_specs=[
            pl.BlockSpec((ROWS, tile_cols, width), lambda step: (step, 0, 0)),
            pl.BlockSpec((hidden, ROWS, tile_cols), lambda step: (0, step, 0)),
            whole((1, hidden)),
            whole((1, hidden)),
            whole((hidden, width)),
        ],
        out_specs=pl.BlockSpec((ROWS, tile_cols, width), lambda step: (step, 0, 0)),
        compiler_params=pltpu.CompilerParams(vmem_limit_bytes=56 * 2**20),
    )(gate, triangle, out_gain[None, :], out_bias[None, :], w_out)


def body(sizes, pair, *rest):
    ny, nx, nz = sizes
    hidden = rest[-1].shape[0]
    tile_rows, tile_cols, _ = pair.shape
    fits = (
        ny == 4
        and hidden % (nx * nz * CHUNKS) == 0
        and hidden % (nx * nz * GROUPS * 8) == 0
        and nx * nz * tile_rows == ny * tile_cols
        and tile_rows % ROWS == 0
        and tile_cols % 128 == 0
        and 2 * 5 * hidden * tile_rows * tile_cols * 2 <= 48 * 2**20
    )
    return channel_body(sizes, pair, *rest) if fits else gather_body(pair, *rest)


def solution(mesh):
    in_specs = (P(("grp", "gx", "gz"), "gy", None), P("grp"), P(), P(), P(), P(), P(), P(), P())
    out_specs = P(("grp", "gx", "gz"), "gy", None)
    sizes = (mesh.shape["gy"], mesh.shape["gx"], mesh.shape["gz"])
    return jax.shard_map(
        functools.partial(body, sizes), mesh=mesh, in_specs=in_specs, out_specs=out_specs, check_vma=False
    )
```

```python
import functools

import jax
import jax.numpy as jnp
from jax import lax
from jax.experimental import pallas as pl
from jax.experimental.pallas import tpu as pltpu
from jax.sharding import PartitionSpec as P

CHUNKS = 32
HEIGHTS = (12, 13, 14, 15, 16)
LAG = 2
DIRECT = 2
GROUPS = 4
ROWS = 32


def layer_norm(values, gain, bias):
    values = values.astype(jnp.float32)
    mean = jnp.mean(values, -1, keepdims=True)
    spread = jnp.mean(jnp.square(values - mean), -1, keepdims=True)
    return (values - mean) * lax.rsqrt(spread + 1e-05) * gain + bias


def channel_norm(values, gain, bias):
    mean = jnp.mean(values, 0, keepdims=True)
    spread = jnp.mean(jnp.square(values - mean), 0, keepdims=True)
    return (values - mean) * lax.rsqrt(spread + 1e-05) * gain[:, None, None] + bias[:, None, None]


def gather_body(pair, lengths, ln_gain, ln_bias, w_ab, w_gate, out_gain, out_bias, w_out):
    tile_rows, tile_cols, width = pair.shape
    hidden = w_out.shape[0]
    row_start = lax.axis_index(("gx", "gz")) * tile_rows
    col_index = lax.axis_index("gy")
    col_start = col_index * tile_cols
    normed = layer_norm(pair, ln_gain, ln_bias).astype(jnp.bfloat16)
    flat = normed.reshape(tile_rows * tile_cols, width)
    proj = jnp.dot(flat, w_ab, preferred_element_type=jnp.float32).reshape(
        tile_rows, tile_cols, 4 * hidden
    )
    row_live = (row_start + jnp.arange(tile_rows, dtype=jnp.int32) < lengths[0]).astype(jnp.float32)
    col_live = (col_start + jnp.arange(tile_cols, dtype=jnp.int32) < lengths[0]).astype(jnp.float32)
    pair_mask = (row_live[:, None] * col_live[None, :])[..., None]
    left = (pair_mask * jax.nn.sigmoid(proj[..., :hidden]) * proj[..., hidden : 2 * hidden]).astype(
        jnp.bfloat16
    )
    right = (
        pair_mask * jax.nn.sigmoid(proj[..., 2 * hidden : 3 * hidden]) * proj[..., 3 * hidden :]
    ).astype(jnp.bfloat16)
    left_major = jnp.transpose(left, (2, 0, 1))
    right_major = jnp.transpose(right, (2, 0, 1))
    column_rows = lax.all_gather(right_major, ("gx", "gz"), axis=1, tiled=True)
    right_mine = lax.all_to_all(column_rows, "gy", split_axis=1, concat_axis=2, tiled=True)
    triangle = jnp.einsum(
        "cik,cjk->cij",
        lax.all_gather(left_major, "gy", axis=2, tiled=True),
        right_mine,
        preferred_element_type=jnp.float32,
    )
    tri_norm = channel_norm(triangle, out_gain, out_bias).astype(jnp.bfloat16)
    gate = jax.nn.sigmoid(jnp.dot(flat, w_gate, preferred_element_type=jnp.float32)).reshape(
        tile_rows, tile_cols, width
    )
    projected = jnp.einsum("cij,cd->ijd", tri_norm, w_out, preferred_element_type=jnp.float32)
    return (gate * projected).astype(jnp.bfloat16)


def exchange_kernel(
    nx,
    nz,
    live,
    lengths,
    pair,
    gain,
    bias,
    w_ab,
    w_gate,
    out,
    gate_out,
    normed,
    send,
    gate_held,
    held,
    given,
    taken,
    operand_send,
    operand_recv,
    pass_send,
    cross_send,
    cross_recv,
    back_send,
    back_recv,
    pair_sem,
    gate_sem,
):
    nr = nx * nz
    hidden, rows, cols = send.shape[1:]
    width = pair.shape[2]
    blocks, lanes = rows // ROWS, ROWS * cols
    each = hidden // nr
    chunks = cross_recv.shape[0]
    part = each // chunks
    gy, gx, gz = lax.axis_index("gy"), lax.axis_index("gx"), lax.axis_index("gz")
    me = gx * nz + gz
    half = gy // 2
    inner_plane, outer_plane = 1 + half, 3 * half
    inner = gy == inner_plane
    outer = jnp.logical_not(inner)

    def place(tall, plane):
        return {"gy": plane, "gx": tall // nz, "gz": tall % nz}

    def remote(src, dst, send_sem, recv_sem, device):
        return pltpu.make_async_remote_copy(
            src_ref=src,
            dst_ref=dst,
            send_sem=send_sem,
            recv_sem=recv_sem,
            device_id=device,
            device_id_type=pl.DeviceIdType.MESH,
        )

    def channels(chunk):
        return pl.ds(chunk * part, part)

    def band(tall):
        return pl.ds(pl.multiple_of(tall * rows, rows), rows)

    def columns(plane):
        return pl.ds(pl.multiple_of((plane - 2 * half) * cols, cols), cols)

    def deal(chunk, step):
        peer = lax.rem(me + step, nr)
        return remote(
            send.at[:, pl.ds(peer * each + chunk * part, part)],
            held.at[:, channels(chunk), band(me), pl.ds(0, cols)],
            operand_send,
            operand_recv.at[chunk],
            place(peer, gy),
        )

    def keep_in(chunk):
        return pltpu.make_async_copy(
            send.at[:, pl.ds(me * each + chunk * part, part)],
            held.at[:, channels(chunk), band(me), pl.ds(0, cols)],
            operand_recv.at[chunk],
        )

    def pass_on(chunk):
        return remote(
            held.at[:, channels(chunk), pl.ds(0, live), pl.ds(0, cols)],
            held.at[:, channels(chunk), pl.ds(0, live), pl.ds(cols, cols)],
            pass_send,
            operand_recv.at[chunk],
            place(me, inner_plane),
        )

    def deal_inward(chunk, step):
        peer = lax.rem(me + step, nr)
        return remote(
            send.at[:, pl.ds(peer * each + chunk * part, part)],
            held.at[:, channels(chunk), band(me), pl.ds(cols, cols)],
            operand_send,
            operand_recv.at[chunk],
            place(peer, inner_plane),
        )

    def cross(chunk):
        return remote(
            given.at[channels(chunk), pl.ds(0, live)],
            taken.at[channels(chunk), pl.ds(0, live)],
            cross_send,
            cross_recv.at[chunk],
            place(me, 3 - gy),
        )

    def hand_back(chunk, step, plane):
        peer = lax.rem(me + step, nr)
        return remote(
            taken.at[channels(chunk), band(peer), columns(plane)],
            out.at[pl.ds(me * each + chunk * part, part)],
            back_send,
            back_recv,
            place(peer, plane),
        )

    def keep_out(chunk):
        return pltpu.make_async_copy(
            taken.at[channels(chunk), band(me), columns(inner_plane)],
            out.at[pl.ds(me * each + chunk * part, part)],
            back_recv,
        )

    def load(block):
        return pltpu.make_async_copy(
            pair.at[pl.ds(block * ROWS, ROWS)],
            normed.at[pl.ds(block * ROWS, ROWS)],
            pair_sem.at[block],
        )

    for block in range(blocks):
        load(block).start()
    barrier = pltpu.get_barrier_semaphore()
    total = 4 * nr
    index = gy * nr + me
    for step in range(1, total):
        peer = lax.rem(index + step, total)
        pl.semaphore_signal(
            barrier,
            inc=1,
            device_id=place(peer % nr, peer // nr),
            device_id_type=pl.DeviceIdType.MESH,
        )

    def take(ref, semaphore):
        pltpu.make_async_copy(ref, ref, semaphore).wait()

    def dealt(chunk, count):
        take(held.at[:, channels(chunk), pl.ds(0, count)], operand_recv.at[chunk])

    side = nr * rows
    if live < side:
        late = slice(DIRECT * part, each)
        held[:, late, live:, cols:] = jnp.zeros((2, each - DIRECT * part, side - live, cols), jnp.bfloat16)

    def product(channel, which):
        below = pl.ds(pl.multiple_of(which * 2 * cols, 2 * cols), 2 * cols)
        return lax.dot_general(
            held[0, channel],
            held[1, channel, below, :],
            (((1,), (1,)), ((), ())),
            preferred_element_type=jnp.float32,
        )

    @pl.loop(0, blocks)
    def _(block):
        load(block).wait()
        here = pl.ds(pl.multiple_of(block * ROWS, ROWS), ROWS)
        flat = normed[here].reshape(lanes, width)
        value = layer_norm(flat, gain[...], bias[...]).astype(jnp.bfloat16)
        normed[here] = value.reshape(ROWS, cols, width)

    upright_w = jnp.transpose(w_ab[...].astype(jnp.float32))
    lane = lax.broadcasted_iota(jnp.int32, (1, lanes), 1)
    col_live = gy * cols + lane % cols < lengths[0]
    span = each // GROUPS

    def project(group):
        starts = [
            kind * hidden + tall * each + group * span for kind in range(4) for tall in range(nr)
        ]
        weights = jnp.concatenate([upright_w[at : at + span] for at in starts]).astype(jnp.bfloat16)
        height = nr * span

        @pl.loop(0, blocks)
        def _(block):
            here = pl.ds(pl.multiple_of(block * ROWS, ROWS), ROWS)
            proj = lax.dot_general(
                weights,
                normed[here].reshape(lanes, width),
                (((1,), (1,)), ((), ())),
                preferred_element_type=jnp.float32,
            )
            row_live = me * rows + block * ROWS + lane // cols < lengths[0]
            mask = (row_live & col_live).astype(jnp.float32)
            for side in range(2):
                gates = proj[2 * side * height : (2 * side + 1) * height]
                values = proj[(2 * side + 1) * height : (2 * side + 2) * height]
                value = mask * jax.nn.sigmoid(gates) * values
                value = value.reshape(height, ROWS, cols).astype(jnp.bfloat16)
                for tall in range(nr):
                    first = tall * each + group * span
                    send[side, first : first + span, here] = value[tall * span : (tall + 1) * span]

        if group == 0:
            pl.semaphore_wait(barrier, total - 1)

        @pl.loop(group * span // part, (group + 1) * span // part)
        def _(chunk):
            direct = outer & (chunk < DIRECT)

            @pl.when(direct)
            def _():
                for step in range(nr):
                    deal_inward(chunk, step).start()

            @pl.when(jnp.logical_not(direct))
            def _():
                for step in range(1, nr):
                    deal(chunk, step).start()
                keep_in(chunk).start()

    for group in range(GROUPS):
        project(group)
        if group:

            @pl.when(outer)
            def _():
                dealt(DIRECT + group - 1, side // 2)
                pass_on(DIRECT + group - 1).start()

    def store_gate(block):
        return pltpu.make_async_copy(
            gate_held.at[block % 2],
            gate_out.at[pl.ds(block * ROWS, ROWS)],
            gate_sem.at[block % 2],
        )

    def gate_turn(turn):
        block = turn - 2 * GROUPS

        @pl.when((block >= 2) & (block < blocks + 2))
        def _():
            store_gate(block - 2).wait()

        @pl.when((block >= 0) & (block < blocks))
        def _():
            here = pl.ds(pl.multiple_of(block * ROWS, ROWS), ROWS)
            value = jax.nn.sigmoid(
                jnp.dot(
                    normed[here].reshape(lanes, width),
                    w_gate[...],
                    preferred_element_type=jnp.float32,
                )
            )
            gate_held[block % 2] = value.reshape(ROWS, cols, width)
            store_gate(block).start()

    @pl.when(outer)
    def _():
        @pl.loop(DIRECT + GROUPS - 1, chunks)
        def _(chunk):
            dealt(chunk, side // 2)
            pass_on(chunk).start()
            gate_turn(chunk)

        take(out, back_recv)
        late = each - DIRECT * part
        take(send.at[:, pl.ds(0, nr * DIRECT * part + (nr - 1) * late)], operand_send)
        take(held.at[:, pl.ds(0, late), pl.ds(0, live), pl.ds(0, cols)], pass_send)

    @pl.when(inner)
    def _():
        @pl.loop(0, chunks + LAG)
        def _(turn):
            @pl.when(turn < chunks)
            def _():
                @pl.when(turn < DIRECT)
                def _():
                    dealt(turn, side)

                @pl.when(turn >= DIRECT)
                def _():
                    dealt(turn, (side + live) // 2)

                @pl.loop(turn * part, (turn + 1) * part)
                def _(channel):
                    given[channel] = product(channel, 1 - half).astype(jnp.bfloat16)

                cross(turn).start()

            @pl.when(turn >= LAG)
            def _():
                chunk = turn - LAG
                cross(chunk).wait_recv()

                @pl.loop(chunk * part, (chunk + 1) * part)
                def _(channel):
                    total = product(channel, half)[:live] + taken[channel, :live].astype(jnp.float32)
                    taken[channel, :live] = total.astype(jnp.bfloat16)
                    if live < side:
                        taken[channel, live:] = jnp.zeros((side - live, 2 * cols), jnp.bfloat16)

                for step in range(nr):
                    hand_back(chunk, step, outer_plane).start()
                for step in range(1, nr):
                    hand_back(chunk, step, inner_plane).start()
                keep_out(chunk).start()

            gate_turn(turn)

        take(out, back_recv)
        take(send.at[:, pl.ds(0, (nr - 1) * each)], operand_send)
        take(given.at[:, pl.ds(0, live)], cross_send)
        take(taken.at[:, pl.ds(0, (2 * nr - 1) * rows // 2)], back_send)


def upright(row):
    return jnp.transpose(jnp.broadcast_to(row[...], (row.shape[1], row.shape[1])))[:, :1]


def finish_kernel(gate, tri, out_gain, out_bias, w_out, out):
    rows, cols, width = out.shape
    hidden = tri.shape[0]
    values = tri[...].astype(jnp.float32)
    mean = jnp.mean(values, 0, keepdims=True)
    centred = values - mean
    spread = jnp.mean(jnp.square(centred), 0, keepdims=True)
    scaled = (centred * lax.rsqrt(spread + 1e-05)).reshape(hidden, rows * cols)
    tri_norm = (scaled * upright(out_gain) + upright(out_bias)).astype(jnp.bfloat16)
    projected = lax.dot_general(
        tri_norm, w_out[...], (((0,), (0,)), ((), ())), preferred_element_type=jnp.float32
    )
    out[...] = (gate[...] * projected.reshape(rows, cols, width)).astype(jnp.bfloat16)


def whole(shape):
    return pl.BlockSpec(shape, lambda step: (0,) * len(shape))


def channel_body(sizes, pair, lengths, ln_gain, ln_bias, w_ab, w_gate, out_gain, out_bias, w_out):
    _, ny, nx, nz = sizes
    tile_rows, tile_cols, width = pair.shape
    hidden = w_out.shape[0]
    gain, bias = ln_gain[None, :], ln_bias[None, :]
    smem = pl.BlockSpec(memory_space=pltpu.SMEM)
    steps = tile_rows // ROWS
    dma = pltpu.SemaphoreType.DMA
    any_space = pl.BlockSpec(memory_space=pl.ANY)
    nr = nx * nz
    each, side = hidden // nr, nr * tile_rows
    vmem = pl.BlockSpec(memory_space=pltpu.VMEM)
    def exchange(variant):
        return pl.pallas_call(
            functools.partial(exchange_kernel, nx, nz, HEIGHTS[variant] * (side // 16)),
            name="exchange",
            out_shape=(
                jax.ShapeDtypeStruct((hidden, tile_rows, tile_cols), jnp.bfloat16),
                jax.ShapeDtypeStruct(pair.shape, jnp.float32),
            ),
            in_specs=[smem, any_space, vmem, vmem, vmem, vmem],
            out_specs=(any_space, any_space),
            scratch_shapes=[
                pltpu.VMEM(pair.shape, jnp.bfloat16),
                pltpu.VMEM((2, hidden, tile_rows, tile_cols), jnp.bfloat16),
                pltpu.VMEM((2, ROWS, tile_cols, width), jnp.float32),
                pltpu.VMEM((2, each, side, 2 * tile_cols), jnp.bfloat16),
                pltpu.VMEM((each, side, 2 * tile_cols), jnp.bfloat16),
                pltpu.VMEM((each, side, 2 * tile_cols), jnp.bfloat16),
                dma,
                dma((CHUNKS,)),
                dma,
                dma,
                dma((CHUNKS,)),
                dma,
                dma,
                dma((steps,)),
                dma((2,)),
            ],
            compiler_params=pltpu.CompilerParams(
                collective_id=variant, has_side_effects=True, vmem_limit_bytes=63 * 2**20
            ),
        )

    longest = jnp.maximum(lengths, lax.ppermute(lengths, "grp", [(0, 1), (1, 0)]))[0]
    variant = jnp.clip((longest - 1) // (side // 16) + 1 - HEIGHTS[0], 0, len(HEIGHTS) - 1)
    triangle, gate = lax.switch(
        variant,
        [exchange(variant) for variant in range(len(HEIGHTS))],
        lengths,
        pair,
        gain,
        bias,
        w_ab,
        w_gate,
    )
    return pl.pallas_call(
        finish_kernel,
        name="finish",
        grid=(steps,),
        out_shape=jax.ShapeDtypeStruct(pair.shape, jnp.bfloat16),
        in_specs=[
            pl.BlockSpec((ROWS, tile_cols, width), lambda step: (step, 0, 0)),
            pl.BlockSpec((hidden, ROWS, tile_cols), lambda step: (0, step, 0)),
            whole((1, hidden)),
            whole((1, hidden)),
            whole((hidden, width)),
        ],
        out_specs=pl.BlockSpec((ROWS, tile_cols, width), lambda step: (step, 0, 0)),
        compiler_params=pltpu.CompilerParams(vmem_limit_bytes=56 * 2**20),
    )(gate, triangle, out_gain[None, :], out_bias[None, :], w_out)


def body(sizes, pair, *rest):
    parts, ny, nx, nz = sizes
    hidden = rest[-1].shape[0]
    tile_rows, tile_cols, _ = pair.shape
    fits = (
        parts == 2
        and ny == 4
        and hidden % (nx * nz * CHUNKS) == 0
        and hidden % (nx * nz * GROUPS * 8) == 0
        and nx * nz * tile_rows == ny * tile_cols
        and tile_rows % ROWS == 0
        and tile_cols % 128 == 0
        and 2 * 5 * hidden * tile_rows * tile_cols * 2 <= 48 * 2**20
    )
    return channel_body(sizes, pair, *rest) if fits else gather_body(pair, *rest)


def solution(mesh):
    in_specs = (P(("grp", "gx", "gz"), "gy", None), P("grp"), P(), P(), P(), P(), P(), P(), P())
    out_specs = P(("grp", "gx", "gz"), "gy", None)
    sizes = tuple(mesh.shape[axis] for axis in ("grp", "gy", "gx", "gz"))
    return jax.shard_map(
        functools.partial(body, sizes), mesh=mesh, in_specs=in_specs, out_specs=out_specs, check_vma=False
    )
```

```python
import functools

import jax
import jax.numpy as jnp
from jax import lax
from jax.experimental import pallas as pl
from jax.experimental.pallas import tpu as pltpu
from jax.sharding import PartitionSpec as P

CHUNKS = 32
LATE = 8
TAIL = 16
HOLD = 3
AHEAD = 8
DIRECT = 1
GROUPS = 4
ROWS = 32
COPIES = 4
HEIGHTS = (12, 13, 14, 15, 16)


def layer_norm(values, gain, bias):
    values = values.astype(jnp.float32)
    mean = jnp.mean(values, -1, keepdims=True)
    spread = jnp.mean(jnp.square(values - mean), -1, keepdims=True)
    return (values - mean) * lax.rsqrt(spread + 1e-05) * gain + bias


def channel_norm(values, gain, bias):
    mean = jnp.mean(values, 0, keepdims=True)
    spread = jnp.mean(jnp.square(values - mean), 0, keepdims=True)
    return (values - mean) * lax.rsqrt(spread + 1e-05) * gain[:, None, None] + bias[:, None, None]


def gather_body(pair, lengths, ln_gain, ln_bias, w_ab, w_gate, out_gain, out_bias, w_out):
    tile_rows, tile_cols, width = pair.shape
    hidden = w_out.shape[0]
    row_start = lax.axis_index(("gx", "gz")) * tile_rows
    col_index = lax.axis_index("gy")
    col_start = col_index * tile_cols
    normed = layer_norm(pair, ln_gain, ln_bias).astype(jnp.bfloat16)
    flat = normed.reshape(tile_rows * tile_cols, width)
    proj = jnp.dot(flat, w_ab, preferred_element_type=jnp.float32).reshape(
        tile_rows, tile_cols, 4 * hidden
    )
    row_live = (row_start + jnp.arange(tile_rows, dtype=jnp.int32) < lengths[0]).astype(jnp.float32)
    col_live = (col_start + jnp.arange(tile_cols, dtype=jnp.int32) < lengths[0]).astype(jnp.float32)
    pair_mask = (row_live[:, None] * col_live[None, :])[..., None]
    left = (pair_mask * jax.nn.sigmoid(proj[..., :hidden]) * proj[..., hidden : 2 * hidden]).astype(
        jnp.bfloat16
    )
    right = (
        pair_mask * jax.nn.sigmoid(proj[..., 2 * hidden : 3 * hidden]) * proj[..., 3 * hidden :]
    ).astype(jnp.bfloat16)
    left_major = jnp.transpose(left, (2, 0, 1))
    right_major = jnp.transpose(right, (2, 0, 1))
    column_rows = lax.all_gather(right_major, ("gx", "gz"), axis=1, tiled=True)
    right_mine = lax.all_to_all(column_rows, "gy", split_axis=1, concat_axis=2, tiled=True)
    triangle = jnp.einsum(
        "cik,cjk->cij",
        lax.all_gather(left_major, "gy", axis=2, tiled=True),
        right_mine,
        preferred_element_type=jnp.float32,
    )
    tri_norm = channel_norm(triangle, out_gain, out_bias).astype(jnp.bfloat16)
    gate = jax.nn.sigmoid(jnp.dot(flat, w_gate, preferred_element_type=jnp.float32)).reshape(
        tile_rows, tile_cols, width
    )
    projected = jnp.einsum("cij,cd->ijd", tri_norm, w_out, preferred_element_type=jnp.float32)
    return (gate * projected).astype(jnp.bfloat16)


def sigmoid_gate(rows, w_gate):
    flat = rows.reshape(rows.shape[0] * rows.shape[1], rows.shape[2])
    return jax.nn.sigmoid(jnp.dot(flat, w_gate, preferred_element_type=jnp.float32))


def upright(row):
    return jnp.transpose(jnp.broadcast_to(row[...], (row.shape[1], row.shape[1])))[:, :1]


def project_out(tri, gain, bias, w_out):
    hidden, rows, cols = tri.shape
    values = tri.astype(jnp.float32)
    mean = jnp.mean(values, 0, keepdims=True)
    centred = values - mean
    spread = jnp.mean(jnp.square(centred), 0, keepdims=True)
    scaled = (centred * lax.rsqrt(spread + 1e-05)).reshape(hidden, rows * cols)
    tri_norm = (scaled * gain + bias).astype(jnp.bfloat16)
    return lax.dot_general(
        tri_norm, w_out, (((0,), (0,)), ((), ())), preferred_element_type=jnp.float32
    )


def pieces(live, bands, rows, first, last):
    full, rest = live // rows, live % rows
    found = [(slice(0, full), slice(first, last))]
    cut = min(max(rest, first), last)
    if cut > first:
        found.append((slice(full, full + 1), slice(first, cut)))
    dead = []
    if full < bands and cut < last:
        dead.append((slice(full, full + 1), slice(cut, last)))
    if full + 1 < bands:
        dead.append((slice(full + 1, bands), slice(first, last)))
    return found, dead


def exchange_kernel(
    nx,
    nz,
    live,
    lengths,
    pair,
    gain,
    bias,
    w_ab,
    w_gate,
    out_gain,
    out_bias,
    w_out,
    done,
    late_tri,
    late_normed,
    normed,
    send,
    held,
    given,
    taken,
    tri,
    staged,
    upright_w,
    extra,
    operand_send,
    operand_recv,
    pass_send,
    cross_send,
    partial_recv,
    late_recv,
    back_send,
    tri_send,
    tri_recv,
    pair_sem,
    done_sem,
):
    nr = nx * nz
    hidden, rows, cols = send.shape[1:]
    width = pair.shape[2]
    blocks, lanes = rows // ROWS, ROWS * cols
    each, side = hidden // nr, nr * rows
    chunks = partial_recv.shape[0]
    part = each // chunks
    late_chunks = late_recv.shape[0]
    late_part = each // late_chunks
    early = rows - TAIL
    gy, gx, gz = lax.axis_index("gy"), lax.axis_index("gx"), lax.axis_index("gz")
    me = gx * nz + gz
    half = gy // 2
    inner_plane, outer_plane = 1 + half, 3 * half
    inner = gy == inner_plane
    outer = jnp.logical_not(inner)

    def place(tall, plane):
        return {"gy": plane, "gx": tall // nz, "gz": tall % nz}

    def remote(src, dst, send_sem, recv_sem, device):
        return pltpu.make_async_remote_copy(
            src_ref=src,
            dst_ref=dst,
            send_sem=send_sem,
            recv_sem=recv_sem,
            device_id=device,
            device_id_type=pl.DeviceIdType.MESH,
        )

    def take(ref, semaphore):
        pltpu.make_async_copy(ref, ref, semaphore).wait()

    def channels(chunk):
        return pl.ds(chunk * part, part)

    def late_channels(chunk):
        return pl.ds(chunk * late_part, late_part)

    def band(tall):
        return pl.ds(pl.multiple_of(tall * rows, rows), rows)

    def columns(plane):
        return pl.ds(pl.multiple_of((plane - 2 * half) * cols, cols), cols)

    def deal(chunk, peer):
        return remote(
            send.at[:, pl.ds(peer * each + chunk * part, part)],
            held.at[:, channels(chunk), band(me), pl.ds(0, cols)],
            operand_send,
            operand_recv.at[chunk],
            place(peer, gy),
        )

    def keep_in(chunk):
        return pltpu.make_async_copy(
            send.at[:, pl.ds(me * each + chunk * part, part)],
            held.at[:, channels(chunk), band(me), pl.ds(0, cols)],
            operand_recv.at[chunk],
        )

    def deal_inward(chunk, peer):
        return remote(
            send.at[:, pl.ds(peer * each + chunk * part, part)],
            held.at[:, channels(chunk), band(me), pl.ds(cols, cols)],
            operand_send,
            operand_recv.at[chunk],
            place(peer, inner_plane),
        )

    def passed(upper):
        if upper:
            return ((0, 0, live), (1, 0, side - rows)) if live > side - rows else ()
        return (0, 0, live), (1, rows, live)

    def passed_rows(upper):
        return sum(last - first for _, first, last in passed(upper))

    def by_half(action):
        for upper in range(2):

            @pl.when(half == upper)
            def _():
                action(upper)

    def pass_on(chunk, upper):
        here = channels(chunk)
        for kind, first, last in passed(upper):
            remote(
                held.at[kind, here, first:last, pl.ds(0, cols)],
                held.at[kind, here, first:last, pl.ds(cols, cols)],
                pass_send,
                operand_recv.at[chunk],
                place(me, inner_plane),
            ).start()

    def cross(here, first, last, semaphore):
        for bands, which in pieces(live, nr, rows, first, last)[0]:
            yield remote(
                given.at[here, bands, which],
                taken.at[here, bands, which],
                cross_send,
                semaphore,
                place(me, 3 - gy),
            )

    def crossed(count, first, last, more):
        return held.at[0, pl.ds(0, count), pl.ds(0, height_of(first, last) + more)]

    def height_of(first, last):
        found = pieces(live, nr, rows, first, last)[0]
        return sum((b.stop - b.start) * (r.stop - r.start) for b, r in found)

    def back(here, which, semaphore):
        return remote(
            taken.at[here, :, which, columns(outer_plane)],
            taken.at[here, :, which, pl.ds(0, cols)],
            back_send,
            semaphore,
            place(me, outer_plane),
        )

    def hand_out(here, which, into, semaphore):
        there = pl.ds(me * each + here.start, here.size)
        for step in range(nr):
            peer = lax.rem(me + step, nr)
            remote(
                taken.at[here, peer, which, columns(outer_plane)],
                into.at[there],
                tri_send,
                semaphore,
                place(peer, outer_plane),
            ).start()

    def hand_back(here, which, into, semaphore, column):
        there = pl.ds(me * each + here.start, here.size)
        for step in range(1, nr):
            peer = lax.rem(me + step, nr)
            remote(
                taken.at[here, peer, which, column],
                into.at[there],
                tri_send,
                semaphore,
                place(peer, gy),
            ).start()
        pltpu.make_async_copy(taken.at[here, me, which, column], into.at[there], semaphore).start()

    def load(block):
        return pltpu.make_async_copy(
            pair.at[pl.ds(block * ROWS, ROWS)],
            normed.at[pl.ds(block * ROWS, ROWS)],
            pair_sem.at[block],
        )

    for block in range(blocks):
        load(block).start()
    barrier = pltpu.get_barrier_semaphore()
    total = 4 * nr
    index = gy * nr + me
    for step in range(1, total):
        peer = lax.rem(index + step, total)
        pl.semaphore_signal(
            barrier,
            inc=1,
            device_id=place(peer % nr, peer // nr),
            device_id_type=pl.DeviceIdType.MESH,
        )

    @pl.loop(0, blocks)
    def _(block):
        load(block).wait()
        here = pl.ds(pl.multiple_of(block * ROWS, ROWS), ROWS)
        flat = normed[here].reshape(lanes, width)
        value = layer_norm(flat, gain[...], bias[...]).astype(jnp.bfloat16)
        normed[here] = value.reshape(ROWS, cols, width)

    upright_w[...] = jnp.transpose(w_ab[...].astype(jnp.float32))
    lane = lax.broadcasted_iota(jnp.int32, (1, lanes), 1)
    col_live = gy * cols + lane % cols < lengths[0]
    span = each // GROUPS

    def project(group):
        starts = [
            pl.multiple_of(kind * hidden + tall * each + group * span, 8)
            for kind in range(4)
            for tall in range(nr)
        ]
        weights = jnp.concatenate([upright_w[pl.ds(at, span)] for at in starts])
        weights = weights.astype(jnp.bfloat16)
        height = nr * span

        @pl.loop(0, blocks)
        def _(block):
            here = pl.ds(pl.multiple_of(block * ROWS, ROWS), ROWS)
            proj = lax.dot_general(
                weights,
                normed[here].reshape(lanes, width),
                (((1,), (1,)), ((), ())),
                preferred_element_type=jnp.float32,
            )
            row_live = me * rows + block * ROWS + lane // cols < lengths[0]
            mask = (row_live & col_live).astype(jnp.float32)
            for kind in range(2):
                gates = proj[2 * kind * height : (2 * kind + 1) * height]
                values = proj[(2 * kind + 1) * height : (2 * kind + 2) * height]
                value = mask * jax.nn.sigmoid(gates) * values
                value = value.reshape(height, ROWS, cols).astype(jnp.bfloat16)
                for tall in range(nr):
                    first = tall * each + group * span
                    send[kind, pl.ds(first, span), here] = value[tall * span : (tall + 1) * span]

        @pl.when(group == 0)
        def _():
            pl.semaphore_wait(barrier, total - 1)

        per_group = span // part
        begin = group * per_group
        first_deals = jnp.where(inner & (group == 1), DIRECT, begin)
        last_deals = jnp.where(inner & (group == 0), DIRECT, begin + per_group)

        @pl.loop(first_deals, last_deals)
        def _(chunk):
            direct = outer & (chunk < DIRECT)

            @pl.when(direct)
            def _():
                for turn in range(nr):
                    deal_inward(chunk, turn % nx * nz + turn // nx).start()

            @pl.when(jnp.logical_not(direct))
            def _():
                for turn in range(nr):
                    peer = turn % nx * nz + turn // nx

                    @pl.when(me != peer)
                    def _():
                        deal(chunk, peer).start()

                keep_in(chunk).start()

    def product(channel, which):
        below = pl.ds(pl.multiple_of(which * 2 * cols, 2 * cols), 2 * cols)
        return lax.dot_general(
            held[0, channel],
            held[1, channel, below, :],
            (((1,), (1,)), ((), ())),
            preferred_element_type=jnp.float32,
        ).reshape(nr, rows, 2 * cols)

    def late_product(channel, below, deep):
        upper = held[0, channel, :, :deep].reshape(nr, rows, deep)[:, early:]
        return lax.dot_general(
            upper.reshape(nr * TAIL, deep),
            held[1, channel, below, :deep],
            (((1,), (1,)), ((), ())),
            preferred_element_type=jnp.float32,
        ).reshape(nr, TAIL, below.size)

    def add(channel, value, first, last):
        found, dead = pieces(live, nr, rows, first, last)
        for bands, which in found:
            inside = slice(which.start - first, which.stop - first)
            known = taken[channel, bands, which].astype(jnp.float32)
            taken[channel, bands, which] = (value[bands, inside] + known).astype(jnp.bfloat16)
        for bands, which in dead:
            shape = (bands.stop - bands.start, which.stop - which.start, 2 * cols)
            taken[channel, bands, which] = jnp.zeros(shape, jnp.bfloat16)

    def collect(chunk):
        @pl.when(chunk < DIRECT)
        def _():
            take(held.at[:, channels(chunk)], operand_recv.at[chunk])

        @pl.when(chunk >= DIRECT)
        def _():
            def wait(upper):
                count = part * (2 * side + passed_rows(upper)) // 32
                take(send.at[0, pl.ds(0, count), pl.ds(0, 32)], operand_recv.at[chunk])

            by_half(wait)

    def front(chunk):
        collect(chunk)

        @pl.loop(chunk * part, (chunk + 1) * part)
        def _(channel):
            given[channel] = product(channel, 1 - half).astype(jnp.bfloat16)

        for copy in cross(channels(chunk), 0, early, partial_recv.at[chunk]):
            copy.start()

    def forward(chunk):
        take(held.at[:, channels(chunk), :, pl.ds(0, cols)], operand_recv.at[chunk])
        by_half(functools.partial(pass_on, chunk))

    @pl.when(inner)
    def _():
        def clear(upper):
            known = dict((kind, (first, last)) for kind, first, last in passed(upper))

            @pl.loop(DIRECT * part, each)
            def _(channel):
                for kind in range(2):
                    first, last = known.get(kind, (0, 0))
                    for begin, end in ((0, first), (last, side)):
                        if begin < end:
                            zero = jnp.zeros((end - begin, cols), jnp.bfloat16)
                            held[kind, channel, begin:end, cols:] = zero

        by_half(clear)

    @pl.loop(0, GROUPS)
    def _(group):
        project(group)

        @pl.when(outer & (group > 0))
        def _():
            forward(DIRECT + group - 1)

        @pl.when(inner & (group > 0))
        def _():
            front(group - 1)

    gains, biases = upright(out_gain), upright(out_bias)

    def store(turn):
        return pltpu.make_async_copy(
            staged.at[turn % 2], done.at[pl.ds(turn * TAIL, TAIL)], done_sem.at[turn % 2]
        )

    def finish(turn):
        @pl.when(turn == 0)
        def _():
            take(tri, tri_recv.at[0])

        @pl.when(turn >= 2)
        def _():
            store(turn - 2).wait()

        here = pl.ds(pl.multiple_of(turn * TAIL, TAIL), TAIL)
        projected = project_out(tri[:, here], gains, biases, w_out[...])
        value = sigmoid_gate(normed[here], w_gate[...]) * projected
        staged[turn % 2] = value.reshape(TAIL, cols, width).astype(jnp.bfloat16)
        store(turn).start()

    turns = early // TAIL

    hold = HOLD if live == side else late_chunks - 2

    def finish_between(chunk):
        share = 2

        @pl.when(chunk >= hold)
        def _():
            begin = jnp.minimum((chunk - hold) * share, turns)
            end = jnp.where(chunk == late_chunks - 1, turns, jnp.minimum(begin + share, turns))

            @pl.loop(begin, end)
            def _(turn):
                finish(turn)

    late_rows = pl.ds(early, TAIL)
    early_rows = pl.ds(0, early)
    keep_normed = pltpu.make_async_copy(normed.at[late_rows], late_normed, done_sem.at[2])
    keep_normed.start()

    @pl.when(outer)
    def _():
        own = band(gy)
        column = pl.ds(0, cols)

        @pl.loop(DIRECT + GROUPS - 1, chunks + AHEAD)
        def _(turn):
            @pl.when(turn < chunks)
            def _():
                forward(turn)

            @pl.when(turn == chunks - 1)
            def _():
                @pl.loop(0, late_chunks)
                def _(chunk):
                    @pl.loop(chunk * late_part, (chunk + 1) * late_part)
                    def _(channel):
                        value = late_product(channel, own, cols).astype(jnp.bfloat16)
                        extra[channel] = value

                    @pl.when(chunk == 0)
                    def _():
                        shape = (DIRECT * part, nr, TAIL, cols)
                        extra[: DIRECT * part] = jnp.zeros(shape, jnp.bfloat16)

                    here = late_channels(chunk)
                    remote(
                        extra.at[here],
                        extra.at[here],
                        cross_send,
                        late_recv.at[chunk],
                        place(me, inner_plane),
                    ).start()

            @pl.when(turn >= AHEAD)
            def _():
                chunk = turn - AHEAD
                here = channels(chunk)
                take(taken.at[here, :, early_rows, column], partial_recv.at[chunk])

                @pl.when(chunk >= DIRECT)
                def _():
                    @pl.loop(chunk * part, (chunk + 1) * part)
                    def _(channel):
                        value = lax.dot_general(
                            held[0, channel, :, :cols],
                            held[1, channel, own, :cols],
                            (((1,), (1,)), ((), ())),
                            preferred_element_type=jnp.float32,
                        ).reshape(nr, rows, cols)[:, :early]
                        value = value + taken[channel, :, :early, :cols].astype(jnp.float32)
                        taken[channel, :, :early, :cols] = value.astype(jnp.bfloat16)

                hand_back(here, early_rows, tri, tri_recv.at[0], column)

        @pl.loop(0, turns)
        def _(turn):
            finish(turn)

        rest = each - DIRECT * part
        take(send.at[:, pl.ds(0, nr * DIRECT * part + (nr - 1) * rest)], operand_send)

        def sent(upper):
            if passed(upper):
                take(held.at[0, pl.ds(0, rest), pl.ds(0, passed_rows(upper) // 2)], pass_send)

        by_half(sent)
        take(extra, cross_send)
        take(held.at[0, :, pl.ds(0, (nr - 1) * early), pl.ds(0, cols)], tri_send)

    @pl.when(inner)
    def _():
        column = columns(inner_plane)
        mine = pl.ds(pl.multiple_of(half * 2 * cols, 2 * cols), 2 * cols)
        outer_column = lax.broadcasted_iota(jnp.int32, (1, 1, 2 * cols), 2) // cols == half

        slowest = max(passed_rows(0), passed_rows(1))
        gap = max(0, slowest - 2 * height_of(0, early)) * chunks * part
        sooner = min(late_chunks, gap // (2 * late_part * height_of(early, rows)))

        @pl.loop(GROUPS - 1, chunks + GROUPS - 1)
        def _(turn):
            @pl.when(turn < chunks)
            def _():
                front(turn)

            @pl.when((turn < sooner * late_part // part) & (turn % (late_part // part) == late_part // part - 1))
            def _():
                chunk = turn // (late_part // part)
                for copy in cross(late_channels(chunk), early, rows, late_recv.at[chunk]):
                    copy.start()

            @pl.when(turn == chunks - 1)
            def _():
                @pl.loop(sooner, late_chunks)
                def _(chunk):
                    for copy in cross(late_channels(chunk), early, rows, late_recv.at[chunk]):
                        copy.start()

            chunk = turn - GROUPS + 1
            here = channels(chunk)
            take(crossed(part, 0, early, 0), partial_recv.at[chunk])

            @pl.loop(chunk * part, (chunk + 1) * part)
            def _(channel):
                add(channel, product(channel, half), 0, early)

            back(here, early_rows, partial_recv.at[chunk]).start()
            hand_back(here, early_rows, tri, tri_recv.at[0], column)

        @pl.loop(0, late_chunks)
        def _(chunk):
            here = late_channels(chunk)
            take(crossed(late_part, early, rows, nr * TAIL // 2), late_recv.at[chunk])

            @pl.loop(chunk * late_part, (chunk + 1) * late_part)
            def _(channel):
                value = late_product(channel, mine, 2 * cols)
                more = extra[channel].astype(jnp.float32)
                more = jnp.where(outer_column, jnp.concatenate([more, more], -1), 0.0)
                add(channel, value + more, early, rows)

            hand_out(here, late_rows, late_tri, tri_recv.at[1])
            hand_back(here, late_rows, late_tri, tri_recv.at[1], column)
            finish_between(chunk)

        take(send.at[:, pl.ds(0, (nr - 1) * each)], operand_send)
        take(held.at[0, :, pl.ds(0, live)], cross_send)
        take(held.at[0, :, pl.ds(0, nr * early), pl.ds(0, cols)], back_send)
        moved = (nr - 1) * early + (2 * nr - 1) * TAIL
        take(held.at[0, :, pl.ds(0, moved), pl.ds(0, cols)], tri_send)

    keep_normed.wait()
    store(turns - 2).wait()
    store(turns - 1).wait()
    take(late_tri, tri_recv.at[1])


def close_kernel(
    done, late_tri, late_normed, w_gate, w_out, out_gain, out_bias, out, whole, tail, flat, weights, sems
):
    early = whole.shape[0]
    step = early // COPIES
    late_loads = [
        pltpu.make_async_copy(late_tri, tail, sems.at[0]),
        pltpu.make_async_copy(late_normed, flat, sems.at[1]),
        pltpu.make_async_copy(w_gate, weights.at[0], sems.at[2]),
        pltpu.make_async_copy(w_out, weights.at[1], sems.at[3]),
    ]
    for copy in late_loads:
        copy.start()
    spans = [pl.ds(turn * step, step) for turn in range(COPIES)]
    loads = [
        pltpu.make_async_copy(done.at[span], whole.at[span], sems.at[4 + turn])
        for turn, span in enumerate(spans)
    ]
    stores = [
        pltpu.make_async_copy(whole.at[span], out.at[span], sems.at[4 + COPIES + turn])
        for turn, span in enumerate(spans)
    ]
    for copy in loads:
        copy.start()
    for load, store in zip(loads, stores):
        load.wait()
        store.start()
    for copy in late_loads:
        copy.wait()
    projected = project_out(tail[...], upright(out_gain), upright(out_bias), weights[1])
    value = sigmoid_gate(flat[...], weights[0]) * projected
    flat[...] = value.reshape(flat.shape).astype(jnp.bfloat16)
    last = pltpu.make_async_copy(flat, out.at[pl.ds(early, flat.shape[0])], sems.at[0])
    last.start()
    for copy in stores:
        copy.wait()
    last.wait()


def channel_body(sizes, pair, lengths, ln_gain, ln_bias, w_ab, w_gate, out_gain, out_bias, w_out):
    _, ny, nx, nz = sizes
    tile_rows, tile_cols, width = pair.shape
    hidden = w_out.shape[0]
    smem = pl.BlockSpec(memory_space=pltpu.SMEM)
    vmem = pl.BlockSpec(memory_space=pltpu.VMEM)
    any_space = pl.BlockSpec(memory_space=pl.ANY)
    dma = pltpu.SemaphoreType.DMA
    steps = tile_rows // ROWS
    nr = nx * nz
    each, side = hidden // nr, nr * tile_rows
    early = tile_rows - TAIL
    half_type = jnp.bfloat16

    def exchange(variant):
        return pl.pallas_call(
            functools.partial(exchange_kernel, nx, nz, HEIGHTS[variant] * (side // 16)),
            name="exchange",
            out_shape=(
                jax.ShapeDtypeStruct(pair.shape, half_type),
                jax.ShapeDtypeStruct((hidden, TAIL, tile_cols), half_type),
                jax.ShapeDtypeStruct((TAIL, tile_cols, width), half_type),
            ),
            in_specs=[smem, any_space] + [vmem] * 7,
            out_specs=(any_space, any_space, any_space),
            scratch_shapes=[
                pltpu.VMEM(pair.shape, half_type),
                pltpu.VMEM((2, hidden, tile_rows, tile_cols), half_type),
                pltpu.VMEM((2, each, side, 2 * tile_cols), half_type),
                pltpu.VMEM((each, nr, tile_rows, 2 * tile_cols), half_type),
                pltpu.VMEM((each, nr, tile_rows, 2 * tile_cols), half_type),
                pltpu.VMEM((hidden, early, tile_cols), half_type),
                pltpu.VMEM((2, TAIL, tile_cols, width), half_type),
                pltpu.VMEM((4 * hidden, width), jnp.float32),
                pltpu.VMEM((each, nr, TAIL, tile_cols), half_type),
                dma,
                dma((CHUNKS,)),
                dma,
                dma,
                dma((CHUNKS,)),
                dma((LATE,)),
                dma,
                dma,
                dma((2,)),
                dma((steps,)),
                dma((3,)),
            ],
            compiler_params=pltpu.CompilerParams(
                collective_id=variant, has_side_effects=True, vmem_limit_bytes=63 * 2**20
            ),
        )

    longest = jnp.maximum(lengths, lax.ppermute(lengths, "grp", [(0, 1), (1, 0)]))[0]
    variant = jnp.clip((longest - 1) // (side // 16) + 1 - HEIGHTS[0], 0, len(HEIGHTS) - 1)
    gains, biases = out_gain[None, :], out_bias[None, :]
    done, late_tri, late_normed = lax.switch(
        variant,
        [exchange(variant) for variant in range(len(HEIGHTS))],
        lengths,
        pair,
        ln_gain[None, :],
        ln_bias[None, :],
        w_ab,
        w_gate,
        gains,
        biases,
        w_out,
    )
    return pl.pallas_call(
        close_kernel,
        name="close",
        out_shape=jax.ShapeDtypeStruct(pair.shape, half_type),
        in_specs=[any_space] * 5 + [vmem] * 2,
        out_specs=any_space,
        scratch_shapes=[
            pltpu.VMEM((early, tile_cols, width), half_type),
            pltpu.VMEM((hidden, TAIL, tile_cols), half_type),
            pltpu.VMEM((TAIL, tile_cols, width), half_type),
            pltpu.VMEM((2,) + w_out.shape, half_type),
            dma((4 + 2 * COPIES,)),
        ],
        compiler_params=pltpu.CompilerParams(vmem_limit_bytes=56 * 2**20),
    )(done, late_tri, late_normed, w_gate, w_out, gains, biases)


def body(sizes, pair, *rest):
    parts, ny, nx, nz = sizes
    hidden = rest[-1].shape[0]
    tile_rows, tile_cols, _ = pair.shape
    fits = (
        parts == 2
        and ny == 4
        and nx * nz == ny
        and hidden % (nx * nz * CHUNKS) == 0
        and hidden % (nx * nz * GROUPS * 8) == 0
        and nx * nz * tile_rows == ny * tile_cols
        and tile_rows == tile_cols
        and tile_cols % 128 == 0
        and 2 * 5 * hidden * tile_rows * tile_cols * 2 <= 48 * 2**20
    )
    return channel_body(sizes, pair, *rest) if fits else gather_body(pair, *rest)


def solution(mesh):
    in_specs = (P(("grp", "gx", "gz"), "gy", None), P("grp"), P(), P(), P(), P(), P(), P(), P())
    out_specs = P(("grp", "gx", "gz"), "gy", None)
    sizes = tuple(mesh.shape[axis] for axis in ("grp", "gy", "gx", "gz"))
    return jax.shard_map(
        functools.partial(body, sizes), mesh=mesh, in_specs=in_specs, out_specs=out_specs, check_vma=False
    )
```

```python
import functools

import jax
import jax.numpy as jnp
from jax import lax
from jax.experimental import pallas as pl
from jax.experimental.pallas import tpu as pltpu
from jax.sharding import PartitionSpec as P

CHUNKS = 32
LATE = 16
TAIL = 16
HOLD = 6
AHEAD = 8
DIRECT = 1
WHOLE = 1
GROUPS = 4
ROWS = 32
NORM_ROWS = 16
COPIES = 4
HEIGHTS = (12, 13, 14, 15, 16)


def layer_norm(values, gain, bias):
    values = values.astype(jnp.float32)
    mean = jnp.mean(values, -1, keepdims=True)
    spread = jnp.mean(jnp.square(values - mean), -1, keepdims=True)
    return (values - mean) * lax.rsqrt(spread + 1e-05) * gain + bias


def channel_norm(values, gain, bias):
    mean = jnp.mean(values, 0, keepdims=True)
    spread = jnp.mean(jnp.square(values - mean), 0, keepdims=True)
    return (values - mean) * lax.rsqrt(spread + 1e-05) * gain[:, None, None] + bias[:, None, None]


def gather_body(pair, lengths, ln_gain, ln_bias, w_ab, w_gate, out_gain, out_bias, w_out):
    tile_rows, tile_cols, width = pair.shape
    hidden = w_out.shape[0]
    row_start = lax.axis_index(("gx", "gz")) * tile_rows
    col_index = lax.axis_index("gy")
    col_start = col_index * tile_cols
    normed = layer_norm(pair, ln_gain, ln_bias).astype(jnp.bfloat16)
    flat = normed.reshape(tile_rows * tile_cols, width)
    proj = jnp.dot(flat, w_ab, preferred_element_type=jnp.float32).reshape(
        tile_rows, tile_cols, 4 * hidden
    )
    row_live = (row_start + jnp.arange(tile_rows, dtype=jnp.int32) < lengths[0]).astype(jnp.float32)
    col_live = (col_start + jnp.arange(tile_cols, dtype=jnp.int32) < lengths[0]).astype(jnp.float32)
    pair_mask = (row_live[:, None] * col_live[None, :])[..., None]
    left = (pair_mask * jax.nn.sigmoid(proj[..., :hidden]) * proj[..., hidden : 2 * hidden]).astype(
        jnp.bfloat16
    )
    right = (
        pair_mask * jax.nn.sigmoid(proj[..., 2 * hidden : 3 * hidden]) * proj[..., 3 * hidden :]
    ).astype(jnp.bfloat16)
    left_major = jnp.transpose(left, (2, 0, 1))
    right_major = jnp.transpose(right, (2, 0, 1))
    column_rows = lax.all_gather(right_major, ("gx", "gz"), axis=1, tiled=True)
    right_mine = lax.all_to_all(column_rows, "gy", split_axis=1, concat_axis=2, tiled=True)
    triangle = jnp.einsum(
        "cik,cjk->cij",
        lax.all_gather(left_major, "gy", axis=2, tiled=True),
        right_mine,
        preferred_element_type=jnp.float32,
    )
    tri_norm = channel_norm(triangle, out_gain, out_bias).astype(jnp.bfloat16)
    gate = jax.nn.sigmoid(jnp.dot(flat, w_gate, preferred_element_type=jnp.float32)).reshape(
        tile_rows, tile_cols, width
    )
    projected = jnp.einsum("cij,cd->ijd", tri_norm, w_out, preferred_element_type=jnp.float32)
    return (gate * projected).astype(jnp.bfloat16)


def sigmoid_gate(rows, w_gate):
    flat = rows.reshape(rows.shape[0] * rows.shape[1], rows.shape[2])
    return jax.nn.sigmoid(jnp.dot(flat, w_gate, preferred_element_type=jnp.float32))


def upright(row):
    return jnp.transpose(jnp.broadcast_to(row[...], (row.shape[1], row.shape[1])))[:, :1]


def project_out(tri, gain, bias, w_out):
    hidden, rows, cols = tri.shape
    values = tri.astype(jnp.float32)
    mean = jnp.mean(values, 0, keepdims=True)
    centred = values - mean
    spread = jnp.mean(jnp.square(centred), 0, keepdims=True)
    scaled = (centred * lax.rsqrt(spread + 1e-05)).reshape(hidden, rows * cols)
    tri_norm = (scaled * gain + bias).astype(jnp.bfloat16)
    return lax.dot_general(
        tri_norm, w_out, (((0,), (0,)), ((), ())), preferred_element_type=jnp.float32
    )


def pieces(live, bands, rows, first, last):
    full, rest = live // rows, live % rows
    found = [(slice(0, full), slice(first, last))]
    cut = min(max(rest, first), last)
    if cut > first:
        found.append((slice(full, full + 1), slice(first, cut)))
    dead = []
    if full < bands and cut < last:
        dead.append((slice(full, full + 1), slice(cut, last)))
    if full + 1 < bands:
        dead.append((slice(full + 1, bands), slice(first, last)))
    return found, dead


def exchange_kernel(
    nx,
    nz,
    live,
    lengths,
    pair,
    *rest,
):
    params, outs, held_params, rest = rest[:7], rest[7:10], rest[10:17], rest[17:]
    done, late_tri, late_normed = outs
    (
        normed,
        send,
        held,
        given,
        taken,
        tri,
        staged,
        upright_w,
        extra,
        operand_send,
        operand_recv,
        pass_send,
        cross_send,
        partial_recv,
        late_recv,
        back_send,
        tri_send,
        tri_recv,
        pair_sem,
        done_sem,
        param_sem,
    ) = rest
    gain, bias, w_ab, w_gate, out_gain, out_bias, w_out = held_params
    nr = nx * nz
    hidden, rows, cols = send.shape[1:]
    width = pair.shape[2]
    blocks = rows // ROWS
    each, side = hidden // nr, nr * rows
    chunks = partial_recv.shape[0]
    part = each // chunks
    late_chunks = late_recv.shape[0]
    late_part = each // late_chunks
    early = rows - TAIL
    gy, gx, gz = lax.axis_index("gy"), lax.axis_index("gx"), lax.axis_index("gz")
    me = gx * nz + gz
    half = gy // 2
    inner_plane, outer_plane = 1 + half, 3 * half
    inner = gy == inner_plane
    outer = jnp.logical_not(inner)

    def place(tall, plane):
        return {"gy": plane, "gx": tall // nz, "gz": tall % nz}

    def remote(src, dst, send_sem, recv_sem, device):
        return pltpu.make_async_remote_copy(
            src_ref=src,
            dst_ref=dst,
            send_sem=send_sem,
            recv_sem=recv_sem,
            device_id=device,
            device_id_type=pl.DeviceIdType.MESH,
        )

    def take(ref, semaphore):
        pltpu.make_async_copy(ref, ref, semaphore).wait()

    def channels(chunk):
        return pl.ds(chunk * part, part)

    def late_channels(chunk):
        return pl.ds(chunk * late_part, late_part)

    def band(tall):
        return pl.ds(pl.multiple_of(tall * rows, rows), rows)

    def columns(plane):
        return pl.ds(pl.multiple_of((plane - 2 * half) * cols, cols), cols)

    def deal(chunk, peer):
        return remote(
            send.at[:, pl.ds(peer * each + chunk * part, part)],
            held.at[:, channels(chunk), band(me), pl.ds(0, cols)],
            operand_send,
            operand_recv.at[chunk],
            place(peer, gy),
        )

    def keep_in(chunk):
        return pltpu.make_async_copy(
            send.at[:, pl.ds(me * each + chunk * part, part)],
            held.at[:, channels(chunk), band(me), pl.ds(0, cols)],
            operand_recv.at[chunk],
        )

    def deal_inward(chunk, peer):
        return remote(
            send.at[:, pl.ds(peer * each + chunk * part, part)],
            held.at[:, channels(chunk), band(me), pl.ds(cols, cols)],
            operand_send,
            operand_recv.at[chunk],
            place(peer, inner_plane),
        )

    settled = chunks - WHOLE
    last_channels = WHOLE * part

    def passed(upper, entire=False):
        if entire:
            return ((0, 0, live), (1, 0, live)) if passed(upper) else ()
        if upper:
            return ((0, 0, live), (1, 0, side - rows)) if live > side - rows else ()
        return (0, 0, live), (1, rows, live)

    def passed_rows(upper, entire=False):
        return sum(last - first for _, first, last in passed(upper, entire))

    def by_half(action):
        for upper in range(2):

            @pl.when(half == upper)
            def _():
                action(upper)

    def pass_on(chunk, entire, upper):
        here = channels(chunk)
        for kind, first, last in passed(upper, entire):
            remote(
                held.at[kind, here, first:last, pl.ds(0, cols)],
                held.at[kind, here, first:last, pl.ds(cols, cols)],
                back_send if entire else pass_send,
                operand_recv.at[chunk],
                place(me, inner_plane),
            ).start()

    def cross(here, first, last, semaphore):
        for bands, which in pieces(live, nr, rows, first, last)[0]:
            yield remote(
                given.at[here, bands, which],
                taken.at[here, bands, which],
                cross_send,
                semaphore,
                place(me, 3 - gy),
            )

    def crossed(count, first, last, more):
        return held.at[0, pl.ds(0, count), pl.ds(0, height_of(first, last) + more)]

    def height_of(first, last):
        found = pieces(live, nr, rows, first, last)[0]
        return sum((b.stop - b.start) * (r.stop - r.start) for b, r in found)

    def back(here, which, semaphore):
        return remote(
            taken.at[here, :, which, columns(outer_plane)],
            taken.at[here, :, which, pl.ds(0, cols)],
            back_send,
            semaphore,
            place(me, outer_plane),
        )

    def hand_out(here, which, into, semaphore, send_semaphore):
        there = pl.ds(me * each + here.start, here.size)
        for step in range(nr):
            peer = lax.rem(me + step, nr)
            remote(
                taken.at[here, peer, which, columns(outer_plane)],
                into.at[there],
                send_semaphore,
                semaphore,
                place(peer, outer_plane),
            ).start()

    def hand_back(here, which, into, semaphore, column):
        there = pl.ds(me * each + here.start, here.size)
        for step in range(1, nr):
            peer = lax.rem(me + step, nr)
            remote(
                taken.at[here, peer, which, column],
                into.at[there],
                tri_send,
                semaphore,
                place(peer, gy),
            ).start()
        pltpu.make_async_copy(taken.at[here, me, which, column], into.at[there], semaphore).start()

    def load(block):
        return pltpu.make_async_copy(
            pair.at[pl.ds(block * NORM_ROWS, NORM_ROWS)],
            normed.at[pl.ds(block * NORM_ROWS, NORM_ROWS)],
            pair_sem.at[block],
        )

    fetches = [
        pltpu.make_async_copy(source, target, param_sem.at[which])
        for which, (source, target) in enumerate(zip(params, held_params))
    ]
    norm_blocks = rows // NORM_ROWS
    load(0).start()
    for fetch in fetches[:3]:
        fetch.start()
    for block in range(1, norm_blocks):
        load(block).start()
    for fetch in fetches[3:]:
        fetch.start()
    barrier = pltpu.get_barrier_semaphore()
    total = 4 * nr
    index = gy * nr + me
    for step in range(1, total):
        peer = lax.rem(index + step, total)
        pl.semaphore_signal(
            barrier,
            inc=1,
            device_id=place(peer % nr, peer // nr),
            device_id_type=pl.DeviceIdType.MESH,
        )

    even = jnp.full((width, width), 1 / width, jnp.bfloat16)
    for fetch in fetches[:3]:
        fetch.wait()
    upright_w[...] = jnp.transpose(w_ab[...].astype(jnp.float32))
    span = each // GROUPS
    height = nr * span

    def norm(block):
        load(block).wait()
        here = pl.ds(pl.multiple_of(block * NORM_ROWS, NORM_ROWS), NORM_ROWS)
        flat = normed[here].reshape(NORM_ROWS * cols, width)
        mean = jnp.dot(flat, even, preferred_element_type=jnp.float32)
        centred = flat.astype(jnp.float32) - mean
        spread = jnp.mean(jnp.square(centred), -1, keepdims=True)
        value = centred * lax.rsqrt(spread + 1e-05) * gain[...] + bias[...]
        normed[here] = value.astype(jnp.bfloat16).reshape(NORM_ROWS, cols, width)

    def weights_of(group):
        starts = [
            pl.multiple_of(kind * hidden + tall * each + group * span, 8)
            for kind in range(4)
            for tall in range(nr)
        ]
        weights = jnp.concatenate([upright_w[pl.ds(at, span)] for at in starts])
        return weights.astype(jnp.bfloat16)

    def project(group, weights, block):
        count = ROWS
        here = pl.ds(pl.multiple_of(block * count, count), count)
        lane = lax.broadcasted_iota(jnp.int32, (1, count * cols), 1)
        proj = lax.dot_general(
            weights,
            normed[here].reshape(count * cols, width),
            (((1,), (1,)), ((), ())),
            preferred_element_type=jnp.float32,
        )
        col_live = gy * cols + lane % cols < lengths[0]
        row_live = me * rows + block * count + lane // cols < lengths[0]
        mask = (row_live & col_live).astype(jnp.float32)
        for kind in range(2):
            gates = proj[2 * kind * height : (2 * kind + 1) * height]
            values = proj[(2 * kind + 1) * height : (2 * kind + 2) * height]
            value = mask * jax.nn.sigmoid(gates) * values
            value = value.reshape(height, count, cols).astype(jnp.bfloat16)
            for tall in range(nr):
                first = tall * each + group * span
                send[kind, pl.ds(first, span), here] = value[tall * span : (tall + 1) * span]

    @pl.loop(0, norm_blocks)
    def _(block):
        norm(block)

    def deals(group):
        @pl.when(group == 0)
        def _():
            pl.semaphore_wait(barrier, total - 1)

        per_group = span // part
        begin = group * per_group
        first_deals = jnp.where(inner & (group == 1), DIRECT, begin)
        last_deals = jnp.where(inner & (group == 0), DIRECT, begin + per_group)

        @pl.loop(first_deals, last_deals)
        def _(chunk):
            direct = outer & (chunk < DIRECT)

            @pl.when(direct)
            def _():
                for turn in range(nr):
                    deal_inward(chunk, turn % nx * nz + turn // nx).start()

            @pl.when(jnp.logical_not(direct))
            def _():
                for turn in range(nr):
                    peer = turn % nx * nz + turn // nx

                    @pl.when(me != peer)
                    def _():
                        deal(chunk, peer).start()

                keep_in(chunk).start()

    def product(channel, which):
        below = pl.ds(pl.multiple_of(which * 2 * cols, 2 * cols), 2 * cols)
        return lax.dot_general(
            held[0, channel],
            held[1, channel, below, :],
            (((1,), (1,)), ((), ())),
            preferred_element_type=jnp.float32,
        ).reshape(nr, rows, 2 * cols)

    def late_product(channel, below, deep):
        upper = held[0, channel, :, :deep].reshape(nr, rows, deep)[:, early:]
        return lax.dot_general(
            upper.reshape(nr * TAIL, deep),
            held[1, channel, below, :deep],
            (((1,), (1,)), ((), ())),
            preferred_element_type=jnp.float32,
        ).reshape(nr, TAIL, below.size)

    def add(channel, value, first, last):
        found, dead = pieces(live, nr, rows, first, last)
        for bands, which in found:
            inside = slice(which.start - first, which.stop - first)
            known = taken[channel, bands, which].astype(jnp.float32)
            taken[channel, bands, which] = (value[bands, inside] + known).astype(jnp.bfloat16)
        for bands, which in dead:
            shape = (bands.stop - bands.start, which.stop - which.start, 2 * cols)
            taken[channel, bands, which] = jnp.zeros(shape, jnp.bfloat16)

    def collect(chunk):
        @pl.when(chunk < DIRECT)
        def _():
            take(held.at[:, channels(chunk)], operand_recv.at[chunk])

        def wait(entire, upper):
            count = part * (2 * side + passed_rows(upper, entire)) // 32
            take(send.at[0, pl.ds(0, count), pl.ds(0, 32)], operand_recv.at[chunk])

        @pl.when((chunk >= DIRECT) & (chunk < settled))
        def _():
            by_half(functools.partial(wait, False))

        @pl.when(chunk >= settled)
        def _():
            by_half(functools.partial(wait, True))

    def front(chunk):
        collect(chunk)

        @pl.loop(chunk * part, (chunk + 1) * part)
        def _(channel):
            given[channel] = product(channel, 1 - half).astype(jnp.bfloat16)

        for copy in cross(channels(chunk), 0, early, partial_recv.at[chunk]):
            copy.start()

    def forward(chunk):
        take(held.at[:, channels(chunk), :, pl.ds(0, cols)], operand_recv.at[chunk])

        @pl.when(chunk < settled)
        def _():
            by_half(functools.partial(pass_on, chunk, False))

        @pl.when(chunk >= settled)
        def _():
            by_half(functools.partial(pass_on, chunk, True))

    @pl.when(inner)
    def _():
        def clear(start, stop, entire, upper):
            known = dict((kind, (first, last)) for kind, first, last in passed(upper, entire))

            @pl.loop(start, stop)
            def _(channel):
                for kind in range(2):
                    first, last = known.get(kind, (0, 0))
                    for begin, end in ((0, first), (last, side)):
                        if begin < end:
                            zero = jnp.zeros((end - begin, cols), jnp.bfloat16)
                            held[kind, channel, begin:end, cols:] = zero

        by_half(functools.partial(clear, DIRECT * part, each - last_channels, False))
        by_half(functools.partial(clear, each - last_channels, each, True))

    @pl.loop(0, GROUPS)
    def _(group):
        weights = weights_of(group)

        @pl.loop(0, blocks)
        def _(block):
            project(group, weights, block)

        deals(group)

        @pl.when(outer & (group > 0))
        def _():
            forward(DIRECT + group - 1)

        @pl.when(inner & (group > 0))
        def _():
            front(group - 1)

    for fetch in fetches[3:]:
        fetch.wait()
    gains, biases = upright(out_gain), upright(out_bias)

    def store(turn):
        return pltpu.make_async_copy(
            staged.at[turn % 2], done.at[pl.ds(turn * TAIL, TAIL)], done_sem.at[turn % 2]
        )

    def finish(turn):
        @pl.when(turn == 0)
        def _():
            take(tri, tri_recv.at[0])

        @pl.when(turn >= 2)
        def _():
            store(turn - 2).wait()

        here = pl.ds(pl.multiple_of(turn * TAIL, TAIL), TAIL)
        projected = project_out(tri[:, here], gains, biases, w_out[...])
        value = sigmoid_gate(normed[here], w_gate[...]) * projected
        staged[turn % 2] = value.reshape(TAIL, cols, width).astype(jnp.bfloat16)
        store(turn).start()

    turns = early // TAIL

    stride = 1 if live == side else 2

    def finish_between(chunk):
        due = chunk - HOLD

        @pl.when((due >= 0) & (due % stride == 0) | (chunk == late_chunks - 1))
        def _():
            begin = jnp.minimum((due + stride - 1) // stride, turns)
            end = jnp.where(chunk == late_chunks - 1, turns, jnp.minimum(begin + 1, turns))

            @pl.loop(begin, end)
            def _(turn):
                finish(turn)

    late_rows = pl.ds(early, TAIL)
    early_rows = pl.ds(0, early)
    keep_normed = pltpu.make_async_copy(normed.at[late_rows], late_normed, done_sem.at[2])
    keep_normed.start()

    @pl.when(outer)
    def _():
        own = band(gy)
        column = pl.ds(0, cols)

        @pl.loop(DIRECT + GROUPS - 1, chunks + AHEAD)
        def _(turn):
            @pl.when(turn < chunks)
            def _():
                forward(turn)

            @pl.when(turn == chunks - 1)
            def _():
                @pl.loop(0, late_chunks)
                def _(chunk):
                    @pl.loop(chunk * late_part, (chunk + 1) * late_part)
                    def _(channel):
                        value = late_product(channel, own, cols).astype(jnp.bfloat16)
                        extra[channel] = value

                    @pl.when(chunk == 0)
                    def _():
                        shape = (DIRECT * part, nr, TAIL, cols)
                        extra[: DIRECT * part] = jnp.zeros(shape, jnp.bfloat16)

                    @pl.when(chunk == late_chunks - 1)
                    def _():
                        shape = (last_channels, nr, TAIL, cols)
                        extra[each - last_channels :] = jnp.zeros(shape, jnp.bfloat16)

                    here = late_channels(chunk)
                    remote(
                        extra.at[here],
                        extra.at[here],
                        cross_send,
                        late_recv.at[chunk],
                        place(me, inner_plane),
                    ).start()

            @pl.when((turn >= AHEAD) & (turn - AHEAD < settled))
            def _():
                chunk = turn - AHEAD
                here = channels(chunk)
                take(taken.at[here, :, early_rows, column], partial_recv.at[chunk])

                @pl.when(chunk >= DIRECT)
                def _():
                    @pl.loop(chunk * part, (chunk + 1) * part)
                    def _(channel):
                        value = lax.dot_general(
                            held[0, channel, :, :cols],
                            held[1, channel, own, :cols],
                            (((1,), (1,)), ((), ())),
                            preferred_element_type=jnp.float32,
                        ).reshape(nr, rows, cols)[:, :early]
                        value = value + taken[channel, :, :early, :cols].astype(jnp.float32)
                        taken[channel, :, :early, :cols] = value.astype(jnp.bfloat16)

                hand_back(here, early_rows, tri, tri_recv.at[0], column)

        @pl.loop(0, turns)
        def _(turn):
            finish(turn)

        rest = each - DIRECT * part
        take(send.at[:, pl.ds(0, nr * DIRECT * part + (nr - 1) * rest)], operand_send)

        def sent(upper):
            if passed(upper):
                kept = rest - last_channels
                take(held.at[0, pl.ds(0, kept), pl.ds(0, passed_rows(upper) // 2)], pass_send)
                take(held.at[0, pl.ds(0, last_channels), pl.ds(0, live)], back_send)

        by_half(sent)
        take(extra, cross_send)
        kept = each - last_channels
        take(held.at[0, pl.ds(0, kept), pl.ds(0, (nr - 1) * early), pl.ds(0, cols)], tri_send)

    @pl.when(inner)
    def _():
        column = columns(inner_plane)
        mine = pl.ds(pl.multiple_of(half * 2 * cols, 2 * cols), 2 * cols)
        outer_column = lax.broadcasted_iota(jnp.int32, (1, 1, 2 * cols), 2) // cols == half

        slowest = max(passed_rows(0), passed_rows(1))
        gap = max(0, slowest - 2 * height_of(0, early)) * chunks * part
        sooner = min(late_chunks - GROUPS, gap // (2 * late_part * height_of(early, rows)))

        @pl.loop(GROUPS - 1, chunks + GROUPS - 1)
        def _(turn):
            @pl.when(turn < chunks)
            def _():
                front(turn)

            ratio = late_part // part
            since = turn - GROUPS + 1

            @pl.when((since < sooner * ratio) & (since % ratio == ratio - 1))
            def _():
                chunk = since // ratio
                for copy in cross(late_channels(chunk), early, rows, late_recv.at[chunk]):
                    copy.start()

            @pl.when(turn == chunks - 1)
            def _():
                @pl.loop(sooner, late_chunks)
                def _(chunk):
                    for copy in cross(late_channels(chunk), early, rows, late_recv.at[chunk]):
                        copy.start()

            chunk = turn - GROUPS + 1
            here = channels(chunk)
            take(crossed(part, 0, early, 0), partial_recv.at[chunk])

            @pl.loop(chunk * part, (chunk + 1) * part)
            def _(channel):
                add(channel, product(channel, half), 0, early)


            @pl.when(chunk < settled)
            def _():
                back(here, early_rows, partial_recv.at[chunk]).start()

            @pl.when(chunk >= settled)
            def _():
                hand_out(here, early_rows, tri, tri_recv.at[0], pass_send)

            hand_back(here, early_rows, tri, tri_recv.at[0], column)

        @pl.loop(0, late_chunks)
        def _(chunk):
            here = late_channels(chunk)
            take(crossed(late_part, early, rows, nr * TAIL // 2), late_recv.at[chunk])

            @pl.loop(chunk * late_part, (chunk + 1) * late_part)
            def _(channel):
                value = late_product(channel, mine, 2 * cols)
                more = extra[channel].astype(jnp.float32)
                more = jnp.where(outer_column, jnp.concatenate([more, more], -1), 0.0)
                add(channel, value + more, early, rows)

            hand_out(here, late_rows, late_tri, tri_recv.at[1], tri_send)
            hand_back(here, late_rows, late_tri, tri_recv.at[1], column)
            finish_between(chunk)

        take(send.at[:, pl.ds(0, (nr - 1) * each)], operand_send)
        take(held.at[0, :, pl.ds(0, live)], cross_send)
        kept = each - last_channels
        take(held.at[0, pl.ds(0, kept), pl.ds(0, nr * early), pl.ds(0, cols)], back_send)
        take(held.at[0, pl.ds(0, last_channels), pl.ds(0, nr * early), pl.ds(0, cols)], pass_send)
        moved = (nr - 1) * early + (2 * nr - 1) * TAIL
        take(held.at[0, :, pl.ds(0, moved), pl.ds(0, cols)], tri_send)

    keep_normed.wait()
    store(turns - 2).wait()
    store(turns - 1).wait()
    take(late_tri, tri_recv.at[1])


def close_kernel(
    done, late_tri, late_normed, w_gate, w_out, out_gain, out_bias, out, whole, tail, flat, weights, sems
):
    early = whole.shape[0]
    step = early // COPIES
    late_loads = [
        pltpu.make_async_copy(late_tri, tail, sems.at[0]),
        pltpu.make_async_copy(late_normed, flat, sems.at[1]),
        pltpu.make_async_copy(w_gate, weights.at[0], sems.at[2]),
        pltpu.make_async_copy(w_out, weights.at[1], sems.at[3]),
    ]
    for copy in late_loads:
        copy.start()
    spans = [pl.ds(turn * step, step) for turn in range(COPIES)]
    loads = [
        pltpu.make_async_copy(done.at[span], whole.at[span], sems.at[4 + turn])
        for turn, span in enumerate(spans)
    ]
    stores = [
        pltpu.make_async_copy(whole.at[span], out.at[span], sems.at[4 + COPIES + turn])
        for turn, span in enumerate(spans)
    ]
    for copy in loads:
        copy.start()
    for load, store in zip(loads, stores):
        load.wait()
        store.start()
    for copy in late_loads:
        copy.wait()
    projected = project_out(tail[...], upright(out_gain), upright(out_bias), weights[1])
    value = sigmoid_gate(flat[...], weights[0]) * projected
    flat[...] = value.reshape(flat.shape).astype(jnp.bfloat16)
    last = pltpu.make_async_copy(flat, out.at[pl.ds(early, flat.shape[0])], sems.at[0])
    last.start()
    for copy in stores:
        copy.wait()
    last.wait()


def channel_body(sizes, pair, lengths, ln_gain, ln_bias, w_ab, w_gate, out_gain, out_bias, w_out):
    _, ny, nx, nz = sizes
    tile_rows, tile_cols, width = pair.shape
    hidden = w_out.shape[0]
    smem = pl.BlockSpec(memory_space=pltpu.SMEM)
    vmem = pl.BlockSpec(memory_space=pltpu.VMEM)
    any_space = pl.BlockSpec(memory_space=pl.ANY)
    dma = pltpu.SemaphoreType.DMA
    nr = nx * nz
    each, side = hidden // nr, nr * tile_rows
    early = tile_rows - TAIL
    half_type = jnp.bfloat16

    gains, biases = out_gain[None, :], out_bias[None, :]
    params = (ln_gain[None, :], ln_bias[None, :], w_ab, w_gate, gains, biases, w_out)

    def exchange(variant):
        return pl.pallas_call(
            functools.partial(exchange_kernel, nx, nz, HEIGHTS[variant] * (side // 16)),
            name="exchange",
            out_shape=(
                jax.ShapeDtypeStruct(pair.shape, half_type),
                jax.ShapeDtypeStruct((hidden, TAIL, tile_cols), half_type),
                jax.ShapeDtypeStruct((TAIL, tile_cols, width), half_type),
            ),
            in_specs=[smem] + [any_space] * 8,
            out_specs=(any_space, any_space, any_space),
            scratch_shapes=[pltpu.VMEM(array.shape, array.dtype) for array in params]
            + [
                pltpu.VMEM(pair.shape, half_type),
                pltpu.VMEM((2, hidden, tile_rows, tile_cols), half_type),
                pltpu.VMEM((2, each, side, 2 * tile_cols), half_type),
                pltpu.VMEM((each, nr, tile_rows, 2 * tile_cols), half_type),
                pltpu.VMEM((each, nr, tile_rows, 2 * tile_cols), half_type),
                pltpu.VMEM((hidden, early, tile_cols), half_type),
                pltpu.VMEM((2, TAIL, tile_cols, width), half_type),
                pltpu.VMEM((4 * hidden, width), jnp.float32),
                pltpu.VMEM((each, nr, TAIL, tile_cols), half_type),
                dma,
                dma((CHUNKS,)),
                dma,
                dma,
                dma((CHUNKS,)),
                dma((LATE,)),
                dma,
                dma,
                dma((2,)),
                dma((tile_rows // NORM_ROWS,)),
                dma((3,)),
                dma((len(params),)),
            ],
            compiler_params=pltpu.CompilerParams(
                collective_id=variant, has_side_effects=True, vmem_limit_bytes=63 * 2**20
            ),
        )

    longest = jnp.maximum(lengths, lax.ppermute(lengths, "grp", [(0, 1), (1, 0)]))[0]
    variant = jnp.clip((longest - 1) // (side // 16) + 1 - HEIGHTS[0], 0, len(HEIGHTS) - 1)
    done, late_tri, late_normed = lax.switch(
        variant,
        [exchange(variant) for variant in range(len(HEIGHTS))],
        lengths,
        pair,
        *params,
    )
    return pl.pallas_call(
        close_kernel,
        name="close",
        out_shape=jax.ShapeDtypeStruct(pair.shape, half_type),
        in_specs=[any_space] * 5 + [vmem] * 2,
        out_specs=any_space,
        scratch_shapes=[
            pltpu.VMEM((early, tile_cols, width), half_type),
            pltpu.VMEM((hidden, TAIL, tile_cols), half_type),
            pltpu.VMEM((TAIL, tile_cols, width), half_type),
            pltpu.VMEM((2,) + w_out.shape, half_type),
            dma((4 + 2 * COPIES,)),
        ],
        compiler_params=pltpu.CompilerParams(vmem_limit_bytes=56 * 2**20),
    )(done, late_tri, late_normed, w_gate, w_out, gains, biases)


def body(sizes, pair, *rest):
    parts, ny, nx, nz = sizes
    hidden = rest[-1].shape[0]
    tile_rows, tile_cols, _ = pair.shape
    fits = (
        parts == 2
        and ny == 4
        and nx * nz == ny
        and hidden % (nx * nz * CHUNKS) == 0
        and hidden % (nx * nz * GROUPS * 8) == 0
        and nx * nz * tile_rows == ny * tile_cols
        and tile_rows == tile_cols
        and tile_cols % 128 == 0
        and 2 * 5 * hidden * tile_rows * tile_cols * 2 <= 48 * 2**20
    )
    return channel_body(sizes, pair, *rest) if fits else gather_body(pair, *rest)


def solution(mesh):
    in_specs = (P(("grp", "gx", "gz"), "gy", None), P("grp"), P(), P(), P(), P(), P(), P(), P())
    out_specs = P(("grp", "gx", "gz"), "gy", None)
    sizes = tuple(mesh.shape[axis] for axis in ("grp", "gy", "gx", "gz"))
    return jax.shard_map(
        functools.partial(body, sizes), mesh=mesh, in_specs=in_specs, out_specs=out_specs, check_vma=False
    )
```

```python
import functools

import jax
import jax.numpy as jnp
from jax import lax
from jax.experimental import pallas as pl
from jax.experimental.pallas import tpu as pltpu
from jax.sharding import PartitionSpec as P

CHUNKS = 32
LATE = 16
TAIL = 16
HOLD = 6
AHEAD = 8
DIRECT = 1
WHOLE = 1
GROUPS = 4
ROWS = 32
NORM_ROWS = 16
COPIES = 4
HEIGHTS = (12, 13, 14, 15, 16)


def layer_norm(values, gain, bias):
    values = values.astype(jnp.float32)
    mean = jnp.mean(values, -1, keepdims=True)
    spread = jnp.mean(jnp.square(values - mean), -1, keepdims=True)
    return (values - mean) * lax.rsqrt(spread + 1e-05) * gain + bias


def channel_norm(values, gain, bias):
    mean = jnp.mean(values, 0, keepdims=True)
    spread = jnp.mean(jnp.square(values - mean), 0, keepdims=True)
    return (values - mean) * lax.rsqrt(spread + 1e-05) * gain[:, None, None] + bias[:, None, None]


def gather_body(pair, lengths, ln_gain, ln_bias, w_ab, w_gate, out_gain, out_bias, w_out):
    tile_rows, tile_cols, width = pair.shape
    hidden = w_out.shape[0]
    row_start = lax.axis_index(("gx", "gz")) * tile_rows
    col_index = lax.axis_index("gy")
    col_start = col_index * tile_cols
    normed = layer_norm(pair, ln_gain, ln_bias).astype(jnp.bfloat16)
    flat = normed.reshape(tile_rows * tile_cols, width)
    proj = jnp.dot(flat, w_ab, preferred_element_type=jnp.float32).reshape(
        tile_rows, tile_cols, 4 * hidden
    )
    row_live = (row_start + jnp.arange(tile_rows, dtype=jnp.int32) < lengths[0]).astype(jnp.float32)
    col_live = (col_start + jnp.arange(tile_cols, dtype=jnp.int32) < lengths[0]).astype(jnp.float32)
    pair_mask = (row_live[:, None] * col_live[None, :])[..., None]
    left = (pair_mask * jax.nn.sigmoid(proj[..., :hidden]) * proj[..., hidden : 2 * hidden]).astype(
        jnp.bfloat16
    )
    right = (
        pair_mask * jax.nn.sigmoid(proj[..., 2 * hidden : 3 * hidden]) * proj[..., 3 * hidden :]
    ).astype(jnp.bfloat16)
    left_major = jnp.transpose(left, (2, 0, 1))
    right_major = jnp.transpose(right, (2, 0, 1))
    column_rows = lax.all_gather(right_major, ("gx", "gz"), axis=1, tiled=True)
    right_mine = lax.all_to_all(column_rows, "gy", split_axis=1, concat_axis=2, tiled=True)
    triangle = jnp.einsum(
        "cik,cjk->cij",
        lax.all_gather(left_major, "gy", axis=2, tiled=True),
        right_mine,
        preferred_element_type=jnp.float32,
    )
    tri_norm = channel_norm(triangle, out_gain, out_bias).astype(jnp.bfloat16)
    gate = jax.nn.sigmoid(jnp.dot(flat, w_gate, preferred_element_type=jnp.float32)).reshape(
        tile_rows, tile_cols, width
    )
    projected = jnp.einsum("cij,cd->ijd", tri_norm, w_out, preferred_element_type=jnp.float32)
    return (gate * projected).astype(jnp.bfloat16)


def sigmoid_gate(rows, w_gate):
    flat = rows.reshape(rows.shape[0] * rows.shape[1], rows.shape[2])
    return jax.nn.sigmoid(jnp.dot(flat, w_gate, preferred_element_type=jnp.float32))


def upright(row):
    return jnp.transpose(jnp.broadcast_to(row[...], (row.shape[1], row.shape[1])))[:, :1]


def project_out(tri, gain, bias, w_out):
    hidden, rows, cols = tri.shape
    values = tri.astype(jnp.float32)
    mean = jnp.mean(values, 0, keepdims=True)
    centred = values - mean
    spread = jnp.mean(jnp.square(centred), 0, keepdims=True)
    scaled = (centred * lax.rsqrt(spread + 1e-05)).reshape(hidden, rows * cols)
    tri_norm = (scaled * gain + bias).astype(jnp.bfloat16)
    return lax.dot_general(
        tri_norm, w_out, (((0,), (0,)), ((), ())), preferred_element_type=jnp.float32
    )


def pieces(live, bands, rows, first, last):
    full, rest = live // rows, live % rows
    found = [(slice(0, full), slice(first, last))]
    cut = min(max(rest, first), last)
    if cut > first:
        found.append((slice(full, full + 1), slice(first, cut)))
    dead = []
    if full < bands and cut < last:
        dead.append((slice(full, full + 1), slice(cut, last)))
    if full + 1 < bands:
        dead.append((slice(full + 1, bands), slice(first, last)))
    return found, dead


def exchange_kernel(
    nx,
    nz,
    live,
    lengths,
    source,
    *rest,
):
    params, outs, held_params, rest = rest[:5], rest[5:7], rest[7:12], rest[12:]
    done, late_tri = outs
    (
        normed,
        send,
        held,
        given,
        taken,
        tri,
        staged,
        extra,
        operand_send,
        operand_recv,
        pass_send,
        cross_send,
        partial_recv,
        late_recv,
        back_send,
        tri_send,
        tri_recv,
        pair_sem,
        done_sem,
        param_sem,
    ) = rest
    upright_w, w_gate, out_gain, out_bias, w_out = held_params
    nr = nx * nz
    hidden, rows, cols = send.shape[1:]
    width = source.shape[2]
    blocks = rows // ROWS
    each, side = hidden // nr, nr * rows
    chunks = partial_recv.shape[0]
    part = each // chunks
    late_chunks = late_recv.shape[0]
    late_part = each // late_chunks
    early = rows - TAIL
    gy, gx, gz = lax.axis_index("gy"), lax.axis_index("gx"), lax.axis_index("gz")
    me = gx * nz + gz
    half = gy // 2
    inner_plane, outer_plane = 1 + half, 3 * half
    inner = gy == inner_plane
    outer = jnp.logical_not(inner)

    def place(tall, plane):
        return {"gy": plane, "gx": tall // nz, "gz": tall % nz}

    def remote(src, dst, send_sem, recv_sem, device):
        return pltpu.make_async_remote_copy(
            src_ref=src,
            dst_ref=dst,
            send_sem=send_sem,
            recv_sem=recv_sem,
            device_id=device,
            device_id_type=pl.DeviceIdType.MESH,
        )

    def take(ref, semaphore):
        pltpu.make_async_copy(ref, ref, semaphore).wait()

    def channels(chunk):
        return pl.ds(chunk * part, part)

    def late_channels(chunk):
        return pl.ds(chunk * late_part, late_part)

    def band(tall):
        return pl.ds(pl.multiple_of(tall * rows, rows), rows)

    def columns(plane):
        return pl.ds(pl.multiple_of((plane - 2 * half) * cols, cols), cols)

    def deal(chunk, peer):
        return remote(
            send.at[:, pl.ds(peer * each + chunk * part, part)],
            held.at[:, channels(chunk), band(me), pl.ds(0, cols)],
            operand_send,
            operand_recv.at[chunk],
            place(peer, gy),
        )

    def keep_in(chunk):
        return pltpu.make_async_copy(
            send.at[:, pl.ds(me * each + chunk * part, part)],
            held.at[:, channels(chunk), band(me), pl.ds(0, cols)],
            operand_recv.at[chunk],
        )

    def deal_inward(chunk, peer):
        return remote(
            send.at[:, pl.ds(peer * each + chunk * part, part)],
            held.at[:, channels(chunk), band(me), pl.ds(cols, cols)],
            operand_send,
            operand_recv.at[chunk],
            place(peer, inner_plane),
        )

    settled = chunks - WHOLE
    last_channels = WHOLE * part

    def passed(upper, entire=False):
        if entire:
            return ((0, 0, live), (1, 0, live)) if passed(upper) else ()
        if upper:
            return ((0, 0, live), (1, 0, side - rows)) if live > side - rows else ()
        return (0, 0, live), (1, rows, live)

    def passed_rows(upper, entire=False):
        return sum(last - first for _, first, last in passed(upper, entire))

    def by_half(action):
        for upper in range(2):

            @pl.when(half == upper)
            def _():
                action(upper)

    def pass_on(chunk, entire, upper):
        here = channels(chunk)
        for kind, first, last in passed(upper, entire):
            remote(
                held.at[kind, here, first:last, pl.ds(0, cols)],
                held.at[kind, here, first:last, pl.ds(cols, cols)],
                back_send if entire else pass_send,
                operand_recv.at[chunk],
                place(me, inner_plane),
            ).start()

    def cross(here, first, last, semaphore):
        for bands, which in pieces(live, nr, rows, first, last)[0]:
            yield remote(
                given.at[here, bands, which],
                taken.at[here, bands, which],
                cross_send,
                semaphore,
                place(me, 3 - gy),
            )

    def crossed(count, first, last, more):
        return held.at[0, pl.ds(0, count), pl.ds(0, height_of(first, last) + more)]

    def height_of(first, last):
        found = pieces(live, nr, rows, first, last)[0]
        return sum((b.stop - b.start) * (r.stop - r.start) for b, r in found)

    def back(here, which, semaphore):
        return remote(
            taken.at[here, :, which, columns(outer_plane)],
            taken.at[here, :, which, pl.ds(0, cols)],
            back_send,
            semaphore,
            place(me, outer_plane),
        )

    def hand_out(here, which, into, semaphore, send_semaphore):
        there = pl.ds(me * each + here.start, here.size)
        for step in range(nr):
            peer = lax.rem(me + step, nr)
            remote(
                taken.at[here, peer, which, columns(outer_plane)],
                into.at[there],
                send_semaphore,
                semaphore,
                place(peer, outer_plane),
            ).start()

    def hand_back(here, which, into, semaphore, column):
        there = pl.ds(me * each + here.start, here.size)
        for step in range(1, nr):
            peer = lax.rem(me + step, nr)
            remote(
                taken.at[here, peer, which, column],
                into.at[there],
                tri_send,
                semaphore,
                place(peer, gy),
            ).start()
        pltpu.make_async_copy(taken.at[here, me, which, column], into.at[there], semaphore).start()

    def load(block):
        return pltpu.make_async_copy(
            source.at[pl.ds(block * ROWS, ROWS)],
            normed.at[pl.ds(block * ROWS, ROWS)],
            pair_sem.at[block],
        )

    fetches = [
        pltpu.make_async_copy(source, target, param_sem.at[which])
        for which, (source, target) in enumerate(zip(params, held_params))
    ]
    fetches[0].start()
    for block in range(blocks):
        load(block).start()
    for fetch in fetches[1:]:
        fetch.start()
    barrier = pltpu.get_barrier_semaphore()
    total = 4 * nr
    index = gy * nr + me
    for step in range(1, total):
        peer = lax.rem(index + step, total)
        pl.semaphore_signal(
            barrier,
            inc=1,
            device_id=place(peer % nr, peer // nr),
            device_id_type=pl.DeviceIdType.MESH,
        )

    span = each // GROUPS
    height = nr * span

    def weights_of(group):
        starts = [
            pl.multiple_of(kind * hidden + tall * each + group * span, 8)
            for kind in range(4)
            for tall in range(nr)
        ]
        weights = jnp.concatenate([upright_w[pl.ds(at, span)] for at in starts])
        return weights.astype(jnp.bfloat16)

    def project(group, weights, block):
        count = ROWS
        here = pl.ds(pl.multiple_of(block * count, count), count)
        lane = lax.broadcasted_iota(jnp.int32, (1, count * cols), 1)
        proj = lax.dot_general(
            weights,
            normed[here].reshape(count * cols, width),
            (((1,), (1,)), ((), ())),
            preferred_element_type=jnp.float32,
        )
        col_live = gy * cols + lane % cols < lengths[0]
        row_live = me * rows + block * count + lane // cols < lengths[0]
        mask = (row_live & col_live).astype(jnp.float32)
        for kind in range(2):
            gates = proj[2 * kind * height : (2 * kind + 1) * height]
            values = proj[(2 * kind + 1) * height : (2 * kind + 2) * height]
            value = mask * jax.nn.sigmoid(gates) * values
            value = value.reshape(height, count, cols).astype(jnp.bfloat16)
            for tall in range(nr):
                first = tall * each + group * span
                send[kind, pl.ds(first, span), here] = value[tall * span : (tall + 1) * span]

    def deals(group):
        @pl.when(group == 0)
        def _():
            pl.semaphore_wait(barrier, total - 1)

        per_group = span // part
        begin = group * per_group
        first_deals = jnp.where(inner & (group == 1), DIRECT, begin)
        last_deals = jnp.where(inner & (group == 0), DIRECT, begin + per_group)

        @pl.loop(first_deals, last_deals)
        def _(chunk):
            direct = outer & (chunk < DIRECT)

            @pl.when(direct)
            def _():
                for turn in range(nr):
                    deal_inward(chunk, turn % nx * nz + turn // nx).start()

            @pl.when(jnp.logical_not(direct))
            def _():
                for turn in range(nr):
                    peer = turn % nx * nz + turn // nx

                    @pl.when(me != peer)
                    def _():
                        deal(chunk, peer).start()

                keep_in(chunk).start()

    def product(channel, which):
        below = pl.ds(pl.multiple_of(which * 2 * cols, 2 * cols), 2 * cols)
        return lax.dot_general(
            held[0, channel],
            held[1, channel, below, :],
            (((1,), (1,)), ((), ())),
            preferred_element_type=jnp.float32,
        ).reshape(nr, rows, 2 * cols)

    def late_product(channel, below, deep):
        upper = held[0, channel, :, :deep].reshape(nr, rows, deep)[:, early:]
        return lax.dot_general(
            upper.reshape(nr * TAIL, deep),
            held[1, channel, below, :deep],
            (((1,), (1,)), ((), ())),
            preferred_element_type=jnp.float32,
        ).reshape(nr, TAIL, below.size)

    def add(channel, value, first, last):
        found, dead = pieces(live, nr, rows, first, last)
        for bands, which in found:
            inside = slice(which.start - first, which.stop - first)
            known = taken[channel, bands, which].astype(jnp.float32)
            taken[channel, bands, which] = (value[bands, inside] + known).astype(jnp.bfloat16)
        for bands, which in dead:
            shape = (bands.stop - bands.start, which.stop - which.start, 2 * cols)
            taken[channel, bands, which] = jnp.zeros(shape, jnp.bfloat16)

    def collect(chunk):
        @pl.when(chunk < DIRECT)
        def _():
            take(held.at[:, channels(chunk)], operand_recv.at[chunk])

        def wait(entire, upper):
            count = part * (2 * side + passed_rows(upper, entire)) // 32
            take(send.at[0, pl.ds(0, count), pl.ds(0, 32)], operand_recv.at[chunk])

        @pl.when((chunk >= DIRECT) & (chunk < settled))
        def _():
            by_half(functools.partial(wait, False))

        @pl.when(chunk >= settled)
        def _():
            by_half(functools.partial(wait, True))

    def front(chunk):
        collect(chunk)

        @pl.loop(chunk * part, (chunk + 1) * part)
        def _(channel):
            given[channel] = product(channel, 1 - half).astype(jnp.bfloat16)

        for copy in cross(channels(chunk), 0, early, partial_recv.at[chunk]):
            copy.start()

    def forward(chunk):
        take(held.at[:, channels(chunk), :, pl.ds(0, cols)], operand_recv.at[chunk])

        @pl.when(chunk < settled)
        def _():
            by_half(functools.partial(pass_on, chunk, False))

        @pl.when(chunk >= settled)
        def _():
            by_half(functools.partial(pass_on, chunk, True))

    @pl.when(inner)
    def _():
        def clear(start, stop, entire, upper):
            known = dict((kind, (first, last)) for kind, first, last in passed(upper, entire))

            @pl.loop(start, stop)
            def _(channel):
                for kind in range(2):
                    first, last = known.get(kind, (0, 0))
                    for begin, end in ((0, first), (last, side)):
                        if begin < end:
                            zero = jnp.zeros((end - begin, cols), jnp.bfloat16)
                            held[kind, channel, begin:end, cols:] = zero

        by_half(functools.partial(clear, DIRECT * part, each - last_channels, False))
        by_half(functools.partial(clear, each - last_channels, each, True))

    fetches[0].wait()

    @pl.loop(0, GROUPS)
    def _(group):
        weights = weights_of(group)

        @pl.loop(0, blocks)
        def _(block):
            @pl.when(group == 0)
            def _():
                load(block).wait()

            project(group, weights, block)

        deals(group)

        @pl.when(outer & (group > 0))
        def _():
            forward(DIRECT + group - 1)

        @pl.when(inner & (group > 0))
        def _():
            front(group - 1)

    for fetch in fetches[1:]:
        fetch.wait()
    gains, biases = upright(out_gain), upright(out_bias)

    def store(turn):
        return pltpu.make_async_copy(
            staged.at[turn % 2], done.at[pl.ds(turn * TAIL, TAIL)], done_sem.at[turn % 2]
        )

    def finish(turn):
        @pl.when(turn == 0)
        def _():
            take(tri, tri_recv.at[0])

        @pl.when(turn >= 2)
        def _():
            store(turn - 2).wait()

        here = pl.ds(pl.multiple_of(turn * TAIL, TAIL), TAIL)
        projected = project_out(tri[:, here], gains, biases, w_out[...])
        value = sigmoid_gate(normed[here], w_gate[...]) * projected
        staged[turn % 2] = value.reshape(TAIL, cols, width).astype(jnp.bfloat16)
        store(turn).start()

    turns = early // TAIL

    stride = 1 if live == side else 2

    def finish_between(chunk):
        due = chunk - HOLD

        @pl.when((due >= 0) & (due % stride == 0) | (chunk == late_chunks - 1))
        def _():
            begin = jnp.minimum((due + stride - 1) // stride, turns)
            end = jnp.where(chunk == late_chunks - 1, turns, jnp.minimum(begin + 1, turns))

            @pl.loop(begin, end)
            def _(turn):
                finish(turn)

    late_rows = pl.ds(early, TAIL)
    early_rows = pl.ds(0, early)

    @pl.when(outer)
    def _():
        own = band(gy)
        column = pl.ds(0, cols)

        @pl.loop(DIRECT + GROUPS - 1, chunks + AHEAD)
        def _(turn):
            @pl.when(turn < chunks)
            def _():
                forward(turn)

            @pl.when(turn == chunks - 1)
            def _():
                @pl.loop(0, late_chunks)
                def _(chunk):
                    @pl.loop(chunk * late_part, (chunk + 1) * late_part)
                    def _(channel):
                        value = late_product(channel, own, cols).astype(jnp.bfloat16)
                        extra[channel] = value

                    @pl.when(chunk == 0)
                    def _():
                        shape = (DIRECT * part, nr, TAIL, cols)
                        extra[: DIRECT * part] = jnp.zeros(shape, jnp.bfloat16)

                    @pl.when(chunk == late_chunks - 1)
                    def _():
                        shape = (last_channels, nr, TAIL, cols)
                        extra[each - last_channels :] = jnp.zeros(shape, jnp.bfloat16)

                    here = late_channels(chunk)
                    remote(
                        extra.at[here],
                        extra.at[here],
                        cross_send,
                        late_recv.at[chunk],
                        place(me, inner_plane),
                    ).start()

            @pl.when((turn >= AHEAD) & (turn - AHEAD < settled))
            def _():
                chunk = turn - AHEAD
                here = channels(chunk)
                take(taken.at[here, :, early_rows, column], partial_recv.at[chunk])

                @pl.when(chunk >= DIRECT)
                def _():
                    @pl.loop(chunk * part, (chunk + 1) * part)
                    def _(channel):
                        value = lax.dot_general(
                            held[0, channel, :, :cols],
                            held[1, channel, own, :cols],
                            (((1,), (1,)), ((), ())),
                            preferred_element_type=jnp.float32,
                        ).reshape(nr, rows, cols)[:, :early]
                        value = value + taken[channel, :, :early, :cols].astype(jnp.float32)
                        taken[channel, :, :early, :cols] = value.astype(jnp.bfloat16)

                hand_back(here, early_rows, tri, tri_recv.at[0], column)

        @pl.loop(0, turns)
        def _(turn):
            finish(turn)

        rest = each - DIRECT * part
        take(send.at[:, pl.ds(0, nr * DIRECT * part + (nr - 1) * rest)], operand_send)

        def sent(upper):
            if passed(upper):
                kept = rest - last_channels
                take(held.at[0, pl.ds(0, kept), pl.ds(0, passed_rows(upper) // 2)], pass_send)
                take(held.at[0, pl.ds(0, last_channels), pl.ds(0, live)], back_send)

        by_half(sent)
        take(extra, cross_send)
        kept = each - last_channels
        take(held.at[0, pl.ds(0, kept), pl.ds(0, (nr - 1) * early), pl.ds(0, cols)], tri_send)

    @pl.when(inner)
    def _():
        column = columns(inner_plane)
        mine = pl.ds(pl.multiple_of(half * 2 * cols, 2 * cols), 2 * cols)
        outer_column = lax.broadcasted_iota(jnp.int32, (1, 1, 2 * cols), 2) // cols == half

        slowest = max(passed_rows(0), passed_rows(1))
        gap = max(0, slowest - 2 * height_of(0, early)) * chunks * part
        sooner = min(late_chunks - GROUPS, gap // (2 * late_part * height_of(early, rows)))

        @pl.loop(GROUPS - 1, chunks + GROUPS - 1)
        def _(turn):
            @pl.when(turn < chunks)
            def _():
                front(turn)

            ratio = late_part // part
            since = turn - GROUPS + 1

            @pl.when((since < sooner * ratio) & (since % ratio == ratio - 1))
            def _():
                chunk = since // ratio
                for copy in cross(late_channels(chunk), early, rows, late_recv.at[chunk]):
                    copy.start()

            @pl.when(turn == chunks - 1)
            def _():
                @pl.loop(sooner, late_chunks)
                def _(chunk):
                    for copy in cross(late_channels(chunk), early, rows, late_recv.at[chunk]):
                        copy.start()

            chunk = turn - GROUPS + 1
            here = channels(chunk)
            take(crossed(part, 0, early, 0), partial_recv.at[chunk])

            @pl.loop(chunk * part, (chunk + 1) * part)
            def _(channel):
                add(channel, product(channel, half), 0, early)


            @pl.when(chunk < settled)
            def _():
                back(here, early_rows, partial_recv.at[chunk]).start()

            @pl.when(chunk >= settled)
            def _():
                hand_out(here, early_rows, tri, tri_recv.at[0], pass_send)

            hand_back(here, early_rows, tri, tri_recv.at[0], column)

        @pl.loop(0, late_chunks)
        def _(chunk):
            here = late_channels(chunk)
            take(crossed(late_part, early, rows, nr * TAIL // 2), late_recv.at[chunk])

            @pl.loop(chunk * late_part, (chunk + 1) * late_part)
            def _(channel):
                value = late_product(channel, mine, 2 * cols)
                more = extra[channel].astype(jnp.float32)
                more = jnp.where(outer_column, jnp.concatenate([more, more], -1), 0.0)
                add(channel, value + more, early, rows)

            hand_out(here, late_rows, late_tri, tri_recv.at[1], tri_send)
            hand_back(here, late_rows, late_tri, tri_recv.at[1], column)
            finish_between(chunk)

        take(send.at[:, pl.ds(0, (nr - 1) * each)], operand_send)
        take(held.at[0, :, pl.ds(0, live)], cross_send)
        kept = each - last_channels
        take(held.at[0, pl.ds(0, kept), pl.ds(0, nr * early), pl.ds(0, cols)], back_send)
        take(held.at[0, pl.ds(0, last_channels), pl.ds(0, nr * early), pl.ds(0, cols)], pass_send)
        moved = (nr - 1) * early + (2 * nr - 1) * TAIL
        take(held.at[0, :, pl.ds(0, moved), pl.ds(0, cols)], tri_send)

    store(turns - 2).wait()
    store(turns - 1).wait()
    take(late_tri, tri_recv.at[1])


def norm_kernel(
    lengths, pair, gain_row, bias_row, w_ab, normed, other, upright_w, flat, gain, bias, weights, turned, sems, link
):
    rows, cols, width = pair.shape
    count = rows // NORM_ROWS
    barrier = pltpu.get_barrier_semaphore()
    far = {"grp": 1 - lax.axis_index("grp")}
    pl.semaphore_signal(barrier, inc=1, device_id=far, device_id_type=pl.DeviceIdType.MESH)

    def span(block):
        return pl.ds(pl.multiple_of(block * NORM_ROWS, NORM_ROWS), NORM_ROWS)

    def load(block):
        return pltpu.make_async_copy(pair.at[span(block)], flat.at[span(block)], sems.at[0, block])

    def store(block):
        return pltpu.make_async_copy(flat.at[span(block)], normed.at[span(block)], sems.at[1, block])

    fetches = [
        pltpu.make_async_copy(source, target, sems.at[2, which])
        for which, (source, target) in enumerate(
            ((gain_row, gain), (bias_row, bias), (w_ab, weights))
        )
    ]
    load(0).start()
    for fetch in fetches:
        fetch.start()
    for block in range(1, count):
        load(block).start()
    for fetch in fetches:
        fetch.wait()
    turned[...] = jnp.transpose(weights[...].astype(jnp.float32))
    keep = pltpu.make_async_copy(turned, upright_w, sems.at[2, 3])
    keep.start()
    even = jnp.full((width, width), 1 / width, jnp.bfloat16)
    tell = pltpu.make_async_remote_copy(
        src_ref=lengths,
        dst_ref=other,
        send_sem=link.at[0],
        recv_sem=link.at[1],
        device_id=far,
        device_id_type=pl.DeviceIdType.MESH,
    )

    def norm(block):
        load(block).wait()
        values = flat[span(block)].reshape(NORM_ROWS * cols, width)
        mean = jnp.dot(values, even, preferred_element_type=jnp.float32)
        centred = values.astype(jnp.float32) - mean
        spread = jnp.mean(jnp.square(centred), -1, keepdims=True)
        value = centred * lax.rsqrt(spread + 1e-05) * gain[...] + bias[...]
        flat[span(block)] = value.astype(jnp.bfloat16).reshape(NORM_ROWS, cols, width)
        store(block).start()

    norm(0)
    pl.semaphore_wait(barrier, 1)
    tell.start()
    pl.loop(1, count)(norm)
    keep.wait()
    tell.wait()

    @pl.loop(0, count)
    def _(block):
        store(block).wait()


def close_kernel(
    done, late_tri, normed, w_gate, w_out, out_gain, out_bias, out, whole, tail, flat, weights, sems
):
    early = whole.shape[0]
    step = early // COPIES
    late_loads = [
        pltpu.make_async_copy(late_tri, tail, sems.at[0]),
        pltpu.make_async_copy(normed.at[pl.ds(early, flat.shape[0])], flat, sems.at[1]),
        pltpu.make_async_copy(w_gate, weights.at[0], sems.at[2]),
        pltpu.make_async_copy(w_out, weights.at[1], sems.at[3]),
    ]
    for copy in late_loads:
        copy.start()
    spans = [pl.ds(turn * step, step) for turn in range(COPIES)]
    loads = [
        pltpu.make_async_copy(done.at[span], whole.at[span], sems.at[4 + turn])
        for turn, span in enumerate(spans)
    ]
    stores = [
        pltpu.make_async_copy(whole.at[span], out.at[span], sems.at[4 + COPIES + turn])
        for turn, span in enumerate(spans)
    ]
    for copy in loads:
        copy.start()
    for load, store in zip(loads, stores):
        load.wait()
        store.start()
    for copy in late_loads:
        copy.wait()
    projected = project_out(tail[...], upright(out_gain), upright(out_bias), weights[1])
    value = sigmoid_gate(flat[...], weights[0]) * projected
    flat[...] = value.reshape(flat.shape).astype(jnp.bfloat16)
    last = pltpu.make_async_copy(flat, out.at[pl.ds(early, flat.shape[0])], sems.at[0])
    last.start()
    for copy in stores:
        copy.wait()
    last.wait()


def channel_body(sizes, pair, lengths, ln_gain, ln_bias, w_ab, w_gate, out_gain, out_bias, w_out):
    _, ny, nx, nz = sizes
    tile_rows, tile_cols, width = pair.shape
    hidden = w_out.shape[0]
    smem = pl.BlockSpec(memory_space=pltpu.SMEM)
    vmem = pl.BlockSpec(memory_space=pltpu.VMEM)
    any_space = pl.BlockSpec(memory_space=pl.ANY)
    dma = pltpu.SemaphoreType.DMA
    nr = nx * nz
    each, side = hidden // nr, nr * tile_rows
    early = tile_rows - TAIL
    half_type = jnp.bfloat16

    gains, biases = out_gain[None, :], out_bias[None, :]
    count = tile_rows // NORM_ROWS
    normed, other, upright_w = pl.pallas_call(
        norm_kernel,
        name="norm",
        out_shape=(
            jax.ShapeDtypeStruct(pair.shape, half_type),
            jax.ShapeDtypeStruct(lengths.shape, lengths.dtype),
            jax.ShapeDtypeStruct((4 * hidden, width), jnp.float32),
        ),
        in_specs=[any_space] * 5,
        out_specs=(any_space,) * 3,
        scratch_shapes=[
            pltpu.VMEM(pair.shape, half_type),
            pltpu.VMEM((1, width), jnp.float32),
            pltpu.VMEM((1, width), jnp.float32),
            pltpu.VMEM(w_ab.shape, half_type),
            pltpu.VMEM((4 * hidden, width), jnp.float32),
            dma((3, max(count, 4))),
            dma((2,)),
        ],
        compiler_params=pltpu.CompilerParams(
            collective_id=len(HEIGHTS), has_side_effects=True, vmem_limit_bytes=63 * 2**20
        ),
    )(lengths, pair, ln_gain[None, :], ln_bias[None, :], w_ab)
    params = (upright_w, w_gate, gains, biases, w_out)

    def exchange(variant):
        return pl.pallas_call(
            functools.partial(exchange_kernel, nx, nz, HEIGHTS[variant] * (side // 16)),
            name="exchange",
            out_shape=(
                jax.ShapeDtypeStruct(pair.shape, half_type),
                jax.ShapeDtypeStruct((hidden, TAIL, tile_cols), half_type),
            ),
            in_specs=[smem] + [any_space] * 6,
            out_specs=(any_space, any_space),
            scratch_shapes=[pltpu.VMEM(array.shape, array.dtype) for array in params]
            + [
                pltpu.VMEM(pair.shape, half_type),
                pltpu.VMEM((2, hidden, tile_rows, tile_cols), half_type),
                pltpu.VMEM((2, each, side, 2 * tile_cols), half_type),
                pltpu.VMEM((each, nr, tile_rows, 2 * tile_cols), half_type),
                pltpu.VMEM((each, nr, tile_rows, 2 * tile_cols), half_type),
                pltpu.VMEM((hidden, early, tile_cols), half_type),
                pltpu.VMEM((2, TAIL, tile_cols, width), half_type),
                pltpu.VMEM((each, nr, TAIL, tile_cols), half_type),
                dma,
                dma((CHUNKS,)),
                dma,
                dma,
                dma((CHUNKS,)),
                dma((LATE,)),
                dma,
                dma,
                dma((2,)),
                dma((tile_rows // ROWS,)),
                dma((2,)),
                dma((len(params),)),
            ],
            compiler_params=pltpu.CompilerParams(
                collective_id=variant, has_side_effects=True, vmem_limit_bytes=63 * 2**20
            ),
        )

    longest = jnp.maximum(lengths, other)[0]
    variant = jnp.clip((longest - 1) // (side // 16) + 1 - HEIGHTS[0], 0, len(HEIGHTS) - 1)
    done, late_tri = lax.switch(
        variant,
        [exchange(variant) for variant in range(len(HEIGHTS))],
        lengths,
        normed,
        *params,
    )
    return pl.pallas_call(
        close_kernel,
        name="close",
        out_shape=jax.ShapeDtypeStruct(pair.shape, half_type),
        in_specs=[any_space] * 5 + [vmem] * 2,
        out_specs=any_space,
        scratch_shapes=[
            pltpu.VMEM((early, tile_cols, width), half_type),
            pltpu.VMEM((hidden, TAIL, tile_cols), half_type),
            pltpu.VMEM((TAIL, tile_cols, width), half_type),
            pltpu.VMEM((2,) + w_out.shape, half_type),
            dma((4 + 2 * COPIES,)),
        ],
        compiler_params=pltpu.CompilerParams(vmem_limit_bytes=56 * 2**20),
    )(done, late_tri, normed, w_gate, w_out, gains, biases)


def body(sizes, pair, *rest):
    parts, ny, nx, nz = sizes
    hidden = rest[-1].shape[0]
    tile_rows, tile_cols, _ = pair.shape
    fits = (
        parts == 2
        and ny == 4
        and nx * nz == ny
        and hidden % (nx * nz * CHUNKS) == 0
        and hidden % (nx * nz * GROUPS * 8) == 0
        and nx * nz * tile_rows == ny * tile_cols
        and tile_rows == tile_cols
        and tile_cols % 128 == 0
        and 2 * 5 * hidden * tile_rows * tile_cols * 2 <= 48 * 2**20
    )
    return channel_body(sizes, pair, *rest) if fits else gather_body(pair, *rest)


def solution(mesh):
    in_specs = (P(("grp", "gx", "gz"), "gy", None), P("grp"), P(), P(), P(), P(), P(), P(), P())
    out_specs = P(("grp", "gx", "gz"), "gy", None)
    sizes = tuple(mesh.shape[axis] for axis in ("grp", "gy", "gx", "gz"))
    return jax.shard_map(
        functools.partial(body, sizes), mesh=mesh, in_specs=in_specs, out_specs=out_specs, check_vma=False
    )
```

```python
import functools

import jax
import jax.numpy as jnp
from jax import lax
from jax.experimental import pallas as pl
from jax.experimental.pallas import tpu as pltpu
from jax.sharding import PartitionSpec as P

CHUNKS = 32
LATE = 16
TAIL = 16
HOLD = 6
AHEAD = 8
DIRECT = 1
WHOLE = 1
GROUPS = 4
ROWS = 32
NORM_ROWS = 16
COPIES = 4
HEIGHTS = (11, 12, 13, 14, 15, 16)


def layer_norm(values, gain, bias):
    values = values.astype(jnp.float32)
    mean = jnp.mean(values, -1, keepdims=True)
    spread = jnp.mean(jnp.square(values - mean), -1, keepdims=True)
    return (values - mean) * lax.rsqrt(spread + 1e-05) * gain + bias


def channel_norm(values, gain, bias):
    mean = jnp.mean(values, 0, keepdims=True)
    spread = jnp.mean(jnp.square(values - mean), 0, keepdims=True)
    return (values - mean) * lax.rsqrt(spread + 1e-05) * gain[:, None, None] + bias[:, None, None]


def gather_body(pair, lengths, ln_gain, ln_bias, w_ab, w_gate, out_gain, out_bias, w_out):
    tile_rows, tile_cols, width = pair.shape
    hidden = w_out.shape[0]
    row_start = lax.axis_index(("gx", "gz")) * tile_rows
    col_index = lax.axis_index("gy")
    col_start = col_index * tile_cols
    normed = layer_norm(pair, ln_gain, ln_bias).astype(jnp.bfloat16)
    flat = normed.reshape(tile_rows * tile_cols, width)
    proj = jnp.dot(flat, w_ab, preferred_element_type=jnp.float32).reshape(
        tile_rows, tile_cols, 4 * hidden
    )
    row_live = (row_start + jnp.arange(tile_rows, dtype=jnp.int32) < lengths[0]).astype(jnp.float32)
    col_live = (col_start + jnp.arange(tile_cols, dtype=jnp.int32) < lengths[0]).astype(jnp.float32)
    pair_mask = (row_live[:, None] * col_live[None, :])[..., None]
    left = (pair_mask * jax.nn.sigmoid(proj[..., :hidden]) * proj[..., hidden : 2 * hidden]).astype(
        jnp.bfloat16
    )
    right = (
        pair_mask * jax.nn.sigmoid(proj[..., 2 * hidden : 3 * hidden]) * proj[..., 3 * hidden :]
    ).astype(jnp.bfloat16)
    left_major = jnp.transpose(left, (2, 0, 1))
    right_major = jnp.transpose(right, (2, 0, 1))
    column_rows = lax.all_gather(right_major, ("gx", "gz"), axis=1, tiled=True)
    right_mine = lax.all_to_all(column_rows, "gy", split_axis=1, concat_axis=2, tiled=True)
    triangle = jnp.einsum(
        "cik,cjk->cij",
        lax.all_gather(left_major, "gy", axis=2, tiled=True),
        right_mine,
        preferred_element_type=jnp.float32,
    )
    tri_norm = channel_norm(triangle, out_gain, out_bias).astype(jnp.bfloat16)
    gate = jax.nn.sigmoid(jnp.dot(flat, w_gate, preferred_element_type=jnp.float32)).reshape(
        tile_rows, tile_cols, width
    )
    projected = jnp.einsum("cij,cd->ijd", tri_norm, w_out, preferred_element_type=jnp.float32)
    return (gate * projected).astype(jnp.bfloat16)


def sigmoid_gate(rows, w_gate):
    flat = rows.reshape(rows.shape[0] * rows.shape[1], rows.shape[2])
    return jax.nn.sigmoid(jnp.dot(flat, w_gate, preferred_element_type=jnp.float32))


def upright(row):
    return jnp.transpose(jnp.broadcast_to(row[...], (row.shape[1], row.shape[1])))[:, :1]


def project_out(tri, gain, bias, w_out):
    hidden, rows, cols = tri.shape
    values = tri.astype(jnp.float32)
    mean = jnp.mean(values, 0, keepdims=True)
    centred = values - mean
    spread = jnp.mean(jnp.square(centred), 0, keepdims=True)
    scaled = (centred * lax.rsqrt(spread + 1e-05)).reshape(hidden, rows * cols)
    tri_norm = (scaled * gain + bias).astype(jnp.bfloat16)
    return lax.dot_general(
        tri_norm, w_out, (((0,), (0,)), ((), ())), preferred_element_type=jnp.float32
    )


def pieces(live, bands, rows, first, last):
    full, rest = live // rows, live % rows
    found = [(slice(0, full), slice(first, last))]
    cut = min(max(rest, first), last)
    if cut > first:
        found.append((slice(full, full + 1), slice(first, cut)))
    dead = []
    if full < bands and cut < last:
        dead.append((slice(full, full + 1), slice(cut, last)))
    if full + 1 < bands:
        dead.append((slice(full + 1, bands), slice(first, last)))
    return found, dead


def exchange_kernel(
    nx,
    nz,
    live,
    lengths,
    source,
    *rest,
):
    params, outs, held_params, rest = rest[:5], rest[5:7], rest[7:12], rest[12:]
    done, late_tri = outs
    (
        normed,
        send,
        held,
        given,
        taken,
        tri,
        staged,
        extra,
        operand_send,
        operand_recv,
        pass_send,
        cross_send,
        partial_recv,
        late_recv,
        back_send,
        tri_send,
        tri_recv,
        pair_sem,
        done_sem,
        param_sem,
    ) = rest
    upright_w, w_gate, out_gain, out_bias, w_out = held_params
    nr = nx * nz
    hidden, rows, cols = send.shape[1:]
    width = source.shape[2]
    blocks = rows // ROWS
    each, side = hidden // nr, nr * rows
    chunks = partial_recv.shape[0]
    part = each // chunks
    late_chunks = late_recv.shape[0]
    late_part = each // late_chunks
    early = rows - TAIL
    gy, gx, gz = lax.axis_index("gy"), lax.axis_index("gx"), lax.axis_index("gz")
    me = gx * nz + gz
    half = gy // 2
    inner_plane, outer_plane = 1 + half, 3 * half
    inner = gy == inner_plane
    outer = jnp.logical_not(inner)

    def place(tall, plane):
        return {"gy": plane, "gx": tall // nz, "gz": tall % nz}

    def remote(src, dst, send_sem, recv_sem, device):
        return pltpu.make_async_remote_copy(
            src_ref=src,
            dst_ref=dst,
            send_sem=send_sem,
            recv_sem=recv_sem,
            device_id=device,
            device_id_type=pl.DeviceIdType.MESH,
        )

    def take(ref, semaphore):
        pltpu.make_async_copy(ref, ref, semaphore).wait()

    def channels(chunk):
        return pl.ds(chunk * part, part)

    def late_channels(chunk):
        return pl.ds(chunk * late_part, late_part)

    def band(tall):
        return pl.ds(pl.multiple_of(tall * rows, rows), rows)

    def columns(plane):
        return pl.ds(pl.multiple_of((plane - 2 * half) * cols, cols), cols)

    def deal(chunk, peer):
        return remote(
            send.at[:, pl.ds(peer * each + chunk * part, part)],
            held.at[:, channels(chunk), band(me), pl.ds(0, cols)],
            operand_send,
            operand_recv.at[chunk],
            place(peer, gy),
        )

    def keep_in(chunk):
        return pltpu.make_async_copy(
            send.at[:, pl.ds(me * each + chunk * part, part)],
            held.at[:, channels(chunk), band(me), pl.ds(0, cols)],
            operand_recv.at[chunk],
        )

    def deal_inward(chunk, peer):
        return remote(
            send.at[:, pl.ds(peer * each + chunk * part, part)],
            held.at[:, channels(chunk), band(me), pl.ds(cols, cols)],
            operand_send,
            operand_recv.at[chunk],
            place(peer, inner_plane),
        )

    settled = chunks - WHOLE
    last_channels = WHOLE * part

    def passed(upper, entire=False):
        if entire:
            return ((0, 0, live), (1, 0, live)) if passed(upper) else ()
        if upper:
            return ((0, 0, live), (1, 0, side - rows)) if live > side - rows else ()
        return (0, 0, live), (1, rows, live)

    def passed_rows(upper, entire=False):
        return sum(last - first for _, first, last in passed(upper, entire))

    def by_half(action):
        for upper in range(2):

            @pl.when(half == upper)
            def _():
                action(upper)

    def pass_on(chunk, entire, upper):
        here = channels(chunk)
        for kind, first, last in passed(upper, entire):
            remote(
                held.at[kind, here, first:last, pl.ds(0, cols)],
                held.at[kind, here, first:last, pl.ds(cols, cols)],
                back_send if entire else pass_send,
                operand_recv.at[chunk],
                place(me, inner_plane),
            ).start()

    def cross(here, first, last, semaphore):
        for bands, which in pieces(live, nr, rows, first, last)[0]:
            yield remote(
                given.at[here, bands, which],
                taken.at[here, bands, which],
                cross_send,
                semaphore,
                place(me, 3 - gy),
            )

    def crossed(count, first, last, more):
        return held.at[0, pl.ds(0, count), pl.ds(0, height_of(first, last) + more)]

    def height_of(first, last):
        found = pieces(live, nr, rows, first, last)[0]
        return sum((b.stop - b.start) * (r.stop - r.start) for b, r in found)

    def back(here, which, semaphore):
        return remote(
            taken.at[here, :, which, columns(outer_plane)],
            taken.at[here, :, which, pl.ds(0, cols)],
            back_send,
            semaphore,
            place(me, outer_plane),
        )

    def hand_out(here, which, into, semaphore, send_semaphore):
        there = pl.ds(me * each + here.start, here.size)
        for step in range(nr):
            peer = lax.rem(me + step, nr)
            remote(
                taken.at[here, peer, which, columns(outer_plane)],
                into.at[there],
                send_semaphore,
                semaphore,
                place(peer, outer_plane),
            ).start()

    def hand_back(here, which, into, semaphore, column):
        there = pl.ds(me * each + here.start, here.size)
        for step in range(1, nr):
            peer = lax.rem(me + step, nr)
            remote(
                taken.at[here, peer, which, column],
                into.at[there],
                tri_send,
                semaphore,
                place(peer, gy),
            ).start()
        pltpu.make_async_copy(taken.at[here, me, which, column], into.at[there], semaphore).start()

    def load(block):
        return pltpu.make_async_copy(
            source.at[pl.ds(block * ROWS, ROWS)],
            normed.at[pl.ds(block * ROWS, ROWS)],
            pair_sem.at[block],
        )

    fetches = [
        pltpu.make_async_copy(source, target, param_sem.at[which])
        for which, (source, target) in enumerate(zip(params, held_params))
    ]
    fetches[0].start()
    for block in range(blocks):
        load(block).start()
    for fetch in fetches[1:]:
        fetch.start()
    barrier = pltpu.get_barrier_semaphore()
    total = 4 * nr
    index = gy * nr + me
    for step in range(1, total):
        peer = lax.rem(index + step, total)
        pl.semaphore_signal(
            barrier,
            inc=1,
            device_id=place(peer % nr, peer // nr),
            device_id_type=pl.DeviceIdType.MESH,
        )

    span = each // GROUPS
    height = nr * span

    def weights_of(group):
        starts = [
            pl.multiple_of(kind * hidden + tall * each + group * span, 8)
            for kind in range(4)
            for tall in range(nr)
        ]
        weights = jnp.concatenate([upright_w[pl.ds(at, span)] for at in starts])
        return weights.astype(jnp.bfloat16)

    def project(group, weights, block):
        count = ROWS
        here = pl.ds(pl.multiple_of(block * count, count), count)
        lane = lax.broadcasted_iota(jnp.int32, (1, count * cols), 1)
        proj = lax.dot_general(
            weights,
            normed[here].reshape(count * cols, width),
            (((1,), (1,)), ((), ())),
            preferred_element_type=jnp.float32,
        )
        col_live = gy * cols + lane % cols < lengths[0]
        row_live = me * rows + block * count + lane // cols < lengths[0]
        mask = (row_live & col_live).astype(jnp.float32)
        for kind in range(2):
            gates = proj[2 * kind * height : (2 * kind + 1) * height]
            values = proj[(2 * kind + 1) * height : (2 * kind + 2) * height]
            value = mask * jax.nn.sigmoid(gates) * values
            value = value.reshape(height, count, cols).astype(jnp.bfloat16)
            for tall in range(nr):
                first = tall * each + group * span
                send[kind, pl.ds(first, span), here] = value[tall * span : (tall + 1) * span]

    def deals(group):
        @pl.when(group == 0)
        def _():
            pl.semaphore_wait(barrier, total - 1)

        per_group = span // part
        begin = group * per_group
        first_deals = jnp.where(inner & (group == 1), DIRECT, begin)
        last_deals = jnp.where(inner & (group == 0), DIRECT, begin + per_group)

        @pl.loop(first_deals, last_deals)
        def _(chunk):
            direct = outer & (chunk < DIRECT)

            @pl.when(direct)
            def _():
                for turn in range(nr):
                    deal_inward(chunk, turn % nx * nz + turn // nx).start()

            @pl.when(jnp.logical_not(direct))
            def _():
                for turn in range(nr):
                    peer = turn % nx * nz + turn // nx

                    @pl.when(me != peer)
                    def _():
                        deal(chunk, peer).start()

                keep_in(chunk).start()

    def product(channel, which):
        below = pl.ds(pl.multiple_of(which * 2 * cols, 2 * cols), 2 * cols)
        return lax.dot_general(
            held[0, channel],
            held[1, channel, below, :],
            (((1,), (1,)), ((), ())),
            preferred_element_type=jnp.float32,
        ).reshape(nr, rows, 2 * cols)

    def late_product(channel, below, deep):
        upper = held[0, channel, :, :deep].reshape(nr, rows, deep)[:, early:]
        return lax.dot_general(
            upper.reshape(nr * TAIL, deep),
            held[1, channel, below, :deep],
            (((1,), (1,)), ((), ())),
            preferred_element_type=jnp.float32,
        ).reshape(nr, TAIL, below.size)

    def add(channel, value, first, last):
        found, dead = pieces(live, nr, rows, first, last)
        for bands, which in found:
            inside = slice(which.start - first, which.stop - first)
            known = taken[channel, bands, which].astype(jnp.float32)
            taken[channel, bands, which] = (value[bands, inside] + known).astype(jnp.bfloat16)
        for bands, which in dead:
            shape = (bands.stop - bands.start, which.stop - which.start, 2 * cols)
            taken[channel, bands, which] = jnp.zeros(shape, jnp.bfloat16)

    def collect(chunk):
        @pl.when(chunk < DIRECT)
        def _():
            take(held.at[:, channels(chunk)], operand_recv.at[chunk])

        def wait(entire, upper):
            count = part * (2 * side + passed_rows(upper, entire)) // 32
            take(send.at[0, pl.ds(0, count), pl.ds(0, 32)], operand_recv.at[chunk])

        @pl.when((chunk >= DIRECT) & (chunk < settled))
        def _():
            by_half(functools.partial(wait, False))

        @pl.when(chunk >= settled)
        def _():
            by_half(functools.partial(wait, True))

    def front(chunk):
        collect(chunk)

        @pl.loop(chunk * part, (chunk + 1) * part)
        def _(channel):
            given[channel] = product(channel, 1 - half).astype(jnp.bfloat16)

        for copy in cross(channels(chunk), 0, early, partial_recv.at[chunk]):
            copy.start()

    def forward(chunk):
        take(held.at[:, channels(chunk), :, pl.ds(0, cols)], operand_recv.at[chunk])

        @pl.when(chunk < settled)
        def _():
            by_half(functools.partial(pass_on, chunk, False))

        @pl.when(chunk >= settled)
        def _():
            by_half(functools.partial(pass_on, chunk, True))

    @pl.when(inner)
    def _():
        def clear(start, stop, entire, upper):
            known = dict((kind, (first, last)) for kind, first, last in passed(upper, entire))

            @pl.loop(start, stop)
            def _(channel):
                for kind in range(2):
                    first, last = known.get(kind, (0, 0))
                    for begin, end in ((0, first), (last, side)):
                        if begin < end:
                            zero = jnp.zeros((end - begin, cols), jnp.bfloat16)
                            held[kind, channel, begin:end, cols:] = zero

        by_half(functools.partial(clear, DIRECT * part, each - last_channels, False))
        by_half(functools.partial(clear, each - last_channels, each, True))

    fetches[0].wait()

    @pl.loop(0, GROUPS)
    def _(group):
        weights = weights_of(group)

        @pl.loop(0, blocks)
        def _(block):
            @pl.when(group == 0)
            def _():
                load(block).wait()

            project(group, weights, block)

        deals(group)

        @pl.when(outer & (group > 0))
        def _():
            forward(DIRECT + group - 1)

        @pl.when(inner & (group > 0))
        def _():
            front(group - 1)

    for fetch in fetches[1:]:
        fetch.wait()
    gains, biases = upright(out_gain), upright(out_bias)

    def store(turn):
        return pltpu.make_async_copy(
            staged.at[turn % 2], done.at[pl.ds(turn * TAIL, TAIL)], done_sem.at[turn % 2]
        )

    def finish(turn):
        @pl.when(turn == 0)
        def _():
            take(tri, tri_recv.at[0])

        @pl.when(turn >= 2)
        def _():
            store(turn - 2).wait()

        here = pl.ds(pl.multiple_of(turn * TAIL, TAIL), TAIL)
        projected = project_out(tri[:, here], gains, biases, w_out[...])
        value = sigmoid_gate(normed[here], w_gate[...]) * projected
        staged[turn % 2] = value.reshape(TAIL, cols, width).astype(jnp.bfloat16)
        store(turn).start()

    turns = early // TAIL

    stride = 1 if live == side else 2

    def finish_between(chunk):
        due = chunk - HOLD

        @pl.when((due >= 0) & (due % stride == 0) | (chunk == late_chunks - 1))
        def _():
            begin = jnp.minimum((due + stride - 1) // stride, turns)
            end = jnp.where(chunk == late_chunks - 1, turns, jnp.minimum(begin + 1, turns))

            @pl.loop(begin, end)
            def _(turn):
                finish(turn)

    late_rows = pl.ds(early, TAIL)
    early_rows = pl.ds(0, early)

    @pl.when(outer)
    def _():
        own = band(gy)
        column = pl.ds(0, cols)

        @pl.loop(DIRECT + GROUPS - 1, chunks + AHEAD)
        def _(turn):
            @pl.when(turn < chunks)
            def _():
                forward(turn)

            @pl.when(turn == chunks - 1)
            def _():
                @pl.loop(0, late_chunks)
                def _(chunk):
                    @pl.loop(chunk * late_part, (chunk + 1) * late_part)
                    def _(channel):
                        value = late_product(channel, own, cols).astype(jnp.bfloat16)
                        extra[channel] = value

                    @pl.when(chunk == 0)
                    def _():
                        shape = (DIRECT * part, nr, TAIL, cols)
                        extra[: DIRECT * part] = jnp.zeros(shape, jnp.bfloat16)

                    @pl.when(chunk == late_chunks - 1)
                    def _():
                        shape = (last_channels, nr, TAIL, cols)
                        extra[each - last_channels :] = jnp.zeros(shape, jnp.bfloat16)

                    here = late_channels(chunk)
                    remote(
                        extra.at[here],
                        extra.at[here],
                        cross_send,
                        late_recv.at[chunk],
                        place(me, inner_plane),
                    ).start()

            @pl.when((turn >= AHEAD) & (turn - AHEAD < settled))
            def _():
                chunk = turn - AHEAD
                here = channels(chunk)
                take(taken.at[here, :, early_rows, column], partial_recv.at[chunk])

                @pl.when(chunk >= DIRECT)
                def _():
                    @pl.loop(chunk * part, (chunk + 1) * part)
                    def _(channel):
                        value = lax.dot_general(
                            held[0, channel, :, :cols],
                            held[1, channel, own, :cols],
                            (((1,), (1,)), ((), ())),
                            preferred_element_type=jnp.float32,
                        ).reshape(nr, rows, cols)[:, :early]
                        value = value + taken[channel, :, :early, :cols].astype(jnp.float32)
                        taken[channel, :, :early, :cols] = value.astype(jnp.bfloat16)

                hand_back(here, early_rows, tri, tri_recv.at[0], column)

        @pl.loop(0, turns)
        def _(turn):
            finish(turn)

        rest = each - DIRECT * part
        take(send.at[:, pl.ds(0, nr * DIRECT * part + (nr - 1) * rest)], operand_send)

        def sent(upper):
            if passed(upper):
                kept = rest - last_channels
                take(held.at[0, pl.ds(0, kept), pl.ds(0, passed_rows(upper) // 2)], pass_send)
                take(held.at[0, pl.ds(0, last_channels), pl.ds(0, live)], back_send)

        by_half(sent)
        take(extra, cross_send)
        kept = each - last_channels
        take(held.at[0, pl.ds(0, kept), pl.ds(0, (nr - 1) * early), pl.ds(0, cols)], tri_send)

    @pl.when(inner)
    def _():
        column = columns(inner_plane)
        mine = pl.ds(pl.multiple_of(half * 2 * cols, 2 * cols), 2 * cols)
        outer_column = lax.broadcasted_iota(jnp.int32, (1, 1, 2 * cols), 2) // cols == half

        slowest = max(passed_rows(0), passed_rows(1))
        gap = max(0, slowest - 2 * height_of(0, early)) * chunks * part
        sooner = min(late_chunks - GROUPS, gap // (2 * late_part * height_of(early, rows)))

        @pl.loop(GROUPS - 1, chunks + GROUPS - 1)
        def _(turn):
            @pl.when(turn < chunks)
            def _():
                front(turn)

            ratio = late_part // part
            since = turn - GROUPS + 1

            @pl.when((since < sooner * ratio) & (since % ratio == ratio - 1))
            def _():
                chunk = since // ratio
                for copy in cross(late_channels(chunk), early, rows, late_recv.at[chunk]):
                    copy.start()

            @pl.when(turn == chunks - 1)
            def _():
                @pl.loop(sooner, late_chunks)
                def _(chunk):
                    for copy in cross(late_channels(chunk), early, rows, late_recv.at[chunk]):
                        copy.start()

            chunk = turn - GROUPS + 1
            here = channels(chunk)
            take(crossed(part, 0, early, 0), partial_recv.at[chunk])

            @pl.loop(chunk * part, (chunk + 1) * part)
            def _(channel):
                add(channel, product(channel, half), 0, early)


            @pl.when(chunk < settled)
            def _():
                back(here, early_rows, partial_recv.at[chunk]).start()

            @pl.when(chunk >= settled)
            def _():
                hand_out(here, early_rows, tri, tri_recv.at[0], pass_send)

            hand_back(here, early_rows, tri, tri_recv.at[0], column)

        @pl.loop(0, late_chunks)
        def _(chunk):
            here = late_channels(chunk)
            take(crossed(late_part, early, rows, nr * TAIL // 2), late_recv.at[chunk])

            @pl.loop(chunk * late_part, (chunk + 1) * late_part)
            def _(channel):
                value = late_product(channel, mine, 2 * cols)
                more = extra[channel].astype(jnp.float32)
                more = jnp.where(outer_column, jnp.concatenate([more, more], -1), 0.0)
                add(channel, value + more, early, rows)

            hand_out(here, late_rows, late_tri, tri_recv.at[1], tri_send)
            hand_back(here, late_rows, late_tri, tri_recv.at[1], column)
            finish_between(chunk)

        take(send.at[:, pl.ds(0, (nr - 1) * each)], operand_send)
        take(held.at[0, :, pl.ds(0, live)], cross_send)
        kept = each - last_channels
        take(held.at[0, pl.ds(0, kept), pl.ds(0, nr * early), pl.ds(0, cols)], back_send)
        take(held.at[0, pl.ds(0, last_channels), pl.ds(0, nr * early), pl.ds(0, cols)], pass_send)
        moved = (nr - 1) * early + (2 * nr - 1) * TAIL
        take(held.at[0, :, pl.ds(0, moved), pl.ds(0, cols)], tri_send)

    store(turns - 2).wait()
    store(turns - 1).wait()
    take(late_tri, tri_recv.at[1])


def norm_kernel(
    lengths, pair, gain_row, bias_row, w_ab, normed, other, upright_w, flat, gain, bias, weights, turned, sems, link
):
    rows, cols, width = pair.shape
    count = rows // NORM_ROWS
    barrier = pltpu.get_barrier_semaphore()
    far = {"grp": 1 - lax.axis_index("grp")}
    pl.semaphore_signal(barrier, inc=1, device_id=far, device_id_type=pl.DeviceIdType.MESH)

    def span(block):
        return pl.ds(pl.multiple_of(block * NORM_ROWS, NORM_ROWS), NORM_ROWS)

    def load(block):
        return pltpu.make_async_copy(pair.at[span(block)], flat.at[span(block)], sems.at[0, block])

    def store(block):
        return pltpu.make_async_copy(flat.at[span(block)], normed.at[span(block)], sems.at[1, block])

    fetches = [
        pltpu.make_async_copy(source, target, sems.at[2, which])
        for which, (source, target) in enumerate(
            ((gain_row, gain), (bias_row, bias), (w_ab, weights))
        )
    ]
    load(0).start()
    for fetch in fetches:
        fetch.start()
    for block in range(1, count):
        load(block).start()
    for fetch in fetches:
        fetch.wait()
    turned[...] = jnp.transpose(weights[...].astype(jnp.float32))
    keep = pltpu.make_async_copy(turned, upright_w, sems.at[2, 3])
    keep.start()
    even = jnp.full((width, width), 1 / width, jnp.bfloat16)
    tell = pltpu.make_async_remote_copy(
        src_ref=lengths,
        dst_ref=other,
        send_sem=link.at[0],
        recv_sem=link.at[1],
        device_id=far,
        device_id_type=pl.DeviceIdType.MESH,
    )

    def norm(block):
        load(block).wait()
        values = flat[span(block)].reshape(NORM_ROWS * cols, width)
        mean = jnp.dot(values, even, preferred_element_type=jnp.float32)
        centred = values.astype(jnp.float32) - mean
        spread = jnp.mean(jnp.square(centred), -1, keepdims=True)
        value = centred * lax.rsqrt(spread + 1e-05) * gain[...] + bias[...]
        flat[span(block)] = value.astype(jnp.bfloat16).reshape(NORM_ROWS, cols, width)
        store(block).start()

    norm(0)
    pl.semaphore_wait(barrier, 1)
    tell.start()
    pl.loop(1, count)(norm)
    keep.wait()
    tell.wait()

    @pl.loop(0, count)
    def _(block):
        store(block).wait()


def close_kernel(
    done, late_tri, normed, w_gate, w_out, out_gain, out_bias, out, whole, tail, flat, weights, sems
):
    early = whole.shape[0]
    step = early // COPIES
    late_loads = [
        pltpu.make_async_copy(late_tri, tail, sems.at[0]),
        pltpu.make_async_copy(normed.at[pl.ds(early, flat.shape[0])], flat, sems.at[1]),
        pltpu.make_async_copy(w_gate, weights.at[0], sems.at[2]),
        pltpu.make_async_copy(w_out, weights.at[1], sems.at[3]),
    ]
    for copy in late_loads:
        copy.start()
    spans = [pl.ds(turn * step, step) for turn in range(COPIES)]
    loads = [
        pltpu.make_async_copy(done.at[span], whole.at[span], sems.at[4 + turn])
        for turn, span in enumerate(spans)
    ]
    stores = [
        pltpu.make_async_copy(whole.at[span], out.at[span], sems.at[4 + COPIES + turn])
        for turn, span in enumerate(spans)
    ]
    for copy in loads:
        copy.start()
    for load, store in zip(loads, stores):
        load.wait()
        store.start()
    for copy in late_loads:
        copy.wait()
    projected = project_out(tail[...], upright(out_gain), upright(out_bias), weights[1])
    value = sigmoid_gate(flat[...], weights[0]) * projected
    flat[...] = value.reshape(flat.shape).astype(jnp.bfloat16)
    last = pltpu.make_async_copy(flat, out.at[pl.ds(early, flat.shape[0])], sems.at[0])
    last.start()
    for copy in stores:
        copy.wait()
    last.wait()


def channel_body(sizes, pair, lengths, ln_gain, ln_bias, w_ab, w_gate, out_gain, out_bias, w_out):
    _, ny, nx, nz = sizes
    tile_rows, tile_cols, width = pair.shape
    hidden = w_out.shape[0]
    smem = pl.BlockSpec(memory_space=pltpu.SMEM)
    vmem = pl.BlockSpec(memory_space=pltpu.VMEM)
    any_space = pl.BlockSpec(memory_space=pl.ANY)
    dma = pltpu.SemaphoreType.DMA
    nr = nx * nz
    each, side = hidden // nr, nr * tile_rows
    early = tile_rows - TAIL
    half_type = jnp.bfloat16

    gains, biases = out_gain[None, :], out_bias[None, :]
    count = tile_rows // NORM_ROWS
    normed, other, upright_w = pl.pallas_call(
        norm_kernel,
        name="norm",
        out_shape=(
            jax.ShapeDtypeStruct(pair.shape, half_type),
            jax.ShapeDtypeStruct(lengths.shape, lengths.dtype),
            jax.ShapeDtypeStruct((4 * hidden, width), jnp.float32),
        ),
        in_specs=[any_space] * 5,
        out_specs=(any_space,) * 3,
        scratch_shapes=[
            pltpu.VMEM(pair.shape, half_type),
            pltpu.VMEM((1, width), jnp.float32),
            pltpu.VMEM((1, width), jnp.float32),
            pltpu.VMEM(w_ab.shape, half_type),
            pltpu.VMEM((4 * hidden, width), jnp.float32),
            dma((3, max(count, 4))),
            dma((2,)),
        ],
        compiler_params=pltpu.CompilerParams(
            collective_id=len(HEIGHTS), has_side_effects=True, vmem_limit_bytes=63 * 2**20
        ),
    )(lengths, pair, ln_gain[None, :], ln_bias[None, :], w_ab)
    params = (upright_w, w_gate, gains, biases, w_out)

    def exchange(variant):
        return pl.pallas_call(
            functools.partial(exchange_kernel, nx, nz, HEIGHTS[variant] * (side // 16)),
            name="exchange",
            out_shape=(
                jax.ShapeDtypeStruct(pair.shape, half_type),
                jax.ShapeDtypeStruct((hidden, TAIL, tile_cols), half_type),
            ),
            in_specs=[smem] + [any_space] * 6,
            out_specs=(any_space, any_space),
            scratch_shapes=[pltpu.VMEM(array.shape, array.dtype) for array in params]
            + [
                pltpu.VMEM(pair.shape, half_type),
                pltpu.VMEM((2, hidden, tile_rows, tile_cols), half_type),
                pltpu.VMEM((2, each, side, 2 * tile_cols), half_type),
                pltpu.VMEM((each, nr, tile_rows, 2 * tile_cols), half_type),
                pltpu.VMEM((each, nr, tile_rows, 2 * tile_cols), half_type),
                pltpu.VMEM((hidden, early, tile_cols), half_type),
                pltpu.VMEM((2, TAIL, tile_cols, width), half_type),
                pltpu.VMEM((each, nr, TAIL, tile_cols), half_type),
                dma,
                dma((CHUNKS,)),
                dma,
                dma,
                dma((CHUNKS,)),
                dma((LATE,)),
                dma,
                dma,
                dma((2,)),
                dma((tile_rows // ROWS,)),
                dma((2,)),
                dma((len(params),)),
            ],
            compiler_params=pltpu.CompilerParams(
                collective_id=variant, has_side_effects=True, vmem_limit_bytes=63 * 2**20
            ),
        )

    longest = jnp.maximum(lengths, other)[0]
    variant = jnp.clip((longest - 1) // (side // 16) + 1 - HEIGHTS[0], 0, len(HEIGHTS) - 1)
    done, late_tri = lax.switch(
        variant,
        [exchange(variant) for variant in range(len(HEIGHTS))],
        lengths,
        normed,
        *params,
    )
    return pl.pallas_call(
        close_kernel,
        name="close",
        out_shape=jax.ShapeDtypeStruct(pair.shape, half_type),
        in_specs=[any_space] * 5 + [vmem] * 2,
        out_specs=any_space,
        scratch_shapes=[
            pltpu.VMEM((early, tile_cols, width), half_type),
            pltpu.VMEM((hidden, TAIL, tile_cols), half_type),
            pltpu.VMEM((TAIL, tile_cols, width), half_type),
            pltpu.VMEM((2,) + w_out.shape, half_type),
            dma((4 + 2 * COPIES,)),
        ],
        compiler_params=pltpu.CompilerParams(vmem_limit_bytes=56 * 2**20),
    )(done, late_tri, normed, w_gate, w_out, gains, biases)


def body(sizes, pair, *rest):
    parts, ny, nx, nz = sizes
    hidden = rest[-1].shape[0]
    tile_rows, tile_cols, _ = pair.shape
    fits = (
        parts == 2
        and ny == 4
        and nx * nz == ny
        and hidden % (nx * nz * CHUNKS) == 0
        and hidden % (nx * nz * GROUPS * 8) == 0
        and nx * nz * tile_rows == ny * tile_cols
        and tile_rows == tile_cols
        and tile_cols % 128 == 0
        and 2 * 5 * hidden * tile_rows * tile_cols * 2 <= 48 * 2**20
    )
    return channel_body(sizes, pair, *rest) if fits else gather_body(pair, *rest)


def solution(mesh):
    in_specs = (P(("grp", "gx", "gz"), "gy", None), P("grp"), P(), P(), P(), P(), P(), P(), P())
    out_specs = P(("grp", "gx", "gz"), "gy", None)
    sizes = tuple(mesh.shape[axis] for axis in ("grp", "gy", "gx", "gz"))
    return jax.shard_map(
        functools.partial(body, sizes), mesh=mesh, in_specs=in_specs, out_specs=out_specs, check_vma=False
    )
```
